128 devices in a mesh: expert: 128 (over y, x, z, core).
Axes of the slice: x: 4, y: 4, z: 4, core: 2. Of those that a mesh axis runs over, the one named last changes fastest.
Arguments:
- tokens: bfloat16 [16384, 4096], P('expert'), may hold values from -6 to 6
- norm_gain: float32 [4096], replicated, may hold values from 0.5 to 1.5
- router_weight: bfloat16 [4096, 128], replicated, may hold values from -0.09375 to 0.09375
- expert_ids: int32 [16384, 2], P('expert'), may hold values from 0 to 127, as said below
- gate_proj: bfloat16 [128, 4096, 768], P('expert'), may hold values from -0.09375 to 0.09375
- up_proj: bfloat16 [128, 4096, 768], P('expert'), may hold values from -0.09375 to 0.09375
- down_proj: bfloat16 [128, 768, 4096], P('expert'), may hold values from -0.21875 to 0.21875
- value_weight: bfloat16 [4096], replicated, may hold values from -0.09375 to 0.09375
- value_target: int32 [16384], P('expert'), may hold values from -1 to 1
- recency: float32 [16384], P('expert'), may hold values from 0.25 to 18, as said below
Outputs:
- mixed: bfloat16 [16384, 4096], P('expert')
- values: float32 [16384], P('expert')
- loss: float32 [], replicated
The draws below stay inside these ranges and needn't reach their ends.
Inputs may be any that keep to these rules, and one draw needn't show every extreme that they name: `expert_ids`: each row names two different experts; among the rows of one device no expert is named more than 3 times. `recency`: positive weights.
All inputs are finite; a program needn't handle non-finite values.
Results may differ from the reference program's by a relative error of at most 0.0055.
Values may be sent and summed in bfloat16 or wider, within the bound.
No kernel may reach another device: no remote copies, remote signals or barrier semaphores. Data moves between devices by JAX's collectives and lax.ppermute only.
A program may use at most 128 MiB of HBM per device.

```python
import jax
import jax.numpy as jnp
from jax import lax

D = 4096
FF = 768
TOK_DEV = 128
EXPERTS = 128
CAP = 3
TOKENS = 16384
N_EXPERT = 128


def draw_expert_ids(key, part):
    key_hot, key_blocks = jax.random.split(jax.random.fold_in(key, 11))
    hottest = jax.random.randint(key_hot, (), 0, EXPERTS)
    block_keys = jax.random.split(key_blocks, TOKENS // TOK_DEV)
    base = jnp.repeat(jnp.arange(EXPERTS - 1, dtype=jnp.int32), CAP, total_repeat_length=(EXPERTS - 1) * CAP)
    others = base + (base >= hottest).astype(jnp.int32)

    def one_block(block_key):
        key_pool, key_rows, key_flip = jax.random.split(block_key, 3)
        shuffled = jax.random.permutation(key_pool, others)
        chosen = shuffled[:2 * TOK_DEV - CAP]
        everything = jnp.concatenate([jnp.full((CAP,), hottest, dtype=jnp.int32), chosen])
        ordered = jnp.sort(everything)
        paired = jnp.stack([ordered[:TOK_DEV], ordered[TOK_DEV:]], axis=1)
        paired = paired[jax.random.permutation(key_rows, TOK_DEV)]
        flipped = jax.random.randint(key_flip, (TOK_DEV, 1), 0, 2)
        return jnp.where(flipped == 1, paired[:, ::-1], paired)
    return lax.map(one_block, block_keys).reshape(TOKENS, 2).astype(jnp.int32)


def draw_recency(key, part):
    position = jnp.arange(TOKENS, dtype=jnp.float32) / TOKENS
    trend = jnp.exp(jnp.log(3.0) * position)
    noise_key = jax.random.fold_in(key, 23)
    noise = jax.random.uniform(noise_key, (TOKENS,), jnp.float32, 0.5, 1.5)
    return (trend * noise).astype(jnp.float32)


def set_ends(entries, key, least, largest):
    index_at = [jax.random.randint(jax.random.fold_in(key, axis), (), 0, length) for axis, length in enumerate(entries.shape)]
    longest = entries.shape.index(max(entries.shape))
    next_to = index_at[:longest] + [(index_at[longest] + 1) % entries.shape[longest]] + index_at[longest + 1:]
    return entries.at[tuple(index_at)].set(least).at[tuple(next_to)].set(largest)


def levels(key, dims, cuts, least, high):
    factor_of, own = 1.0, jax.random.fold_in(key, 6)
    for dim, parts in cuts:
        steps = jnp.exp(jax.random.uniform(jax.random.fold_in(own, dim), (parts,), jnp.float32, least / len(cuts), high / len(cuts)))
        factor_of = factor_of * jnp.repeat(steps, dims[dim] // parts).reshape([-1 if axis == dim else 1 for axis in range(len(dims))])
    return factor_of


def scatter_about(rng, extent, width, most, cuts=(), held_as=jnp.bfloat16):
    array = jax.random.normal(rng, extent, jnp.float32) * width
    if len(cuts) > 0:
        array = levels(rng, extent, cuts, -0.22, 0.18) * array
    return jnp.clip(array, min=-most, max=most).astype(held_as)


def setup_inputs(seed: int = 0) -> dict:
    seeds = jax.random.split(jax.random.key(seed), 11)
    tokens = scatter_about(seeds[0], (TOKENS, D), 1.0, 6.0, ((0, 128),))
    norm_gain = jnp.clip(1.0 + 0.1 * jax.random.normal(seeds[1], (D,), jnp.float32), 0.5, 1.5)
    router_weight = scatter_about(seeds[2], (D, EXPERTS), D ** -0.5, 0.09375)
    expert_ids = draw_expert_ids(jax.random.fold_in(seeds[10], 71), 0)
    gate_proj = scatter_about(seeds[4], (EXPERTS, D, FF), D ** -0.5, 0.09375, ((0, 128),))
    up_proj = scatter_about(seeds[5], (EXPERTS, D, FF), D ** -0.5, 0.09375, ((0, 128),))
    down_proj = scatter_about(seeds[6], (EXPERTS, FF, D), FF ** -0.5, 0.21875, ((0, 128),))
    value_weight = scatter_about(seeds[7], (D,), D ** -0.5, 0.09375)
    value_target = set_ends(jax.random.randint(seeds[8], (TOKENS,), -1, 2), jax.random.fold_in(seeds[8], 1), -1, 1).astype(jnp.int32)
    recency = draw_recency(jax.random.fold_in(seeds[10], 71), 0)
    return dict(tokens=tokens, norm_gain=norm_gain, router_weight=router_weight, expert_ids=expert_ids, gate_proj=gate_proj, up_proj=up_proj, down_proj=down_proj, value_weight=value_weight, value_target=value_target, recency=recency)


def block_ranks(flat_ids):
    columns = jnp.arange(EXPERTS, dtype=jnp.int32)
    one_hot = (flat_ids[:, None] == columns[None, :]).astype(jnp.int32)
    return lax.optimization_barrier(jnp.sum(jnp.cumsum(one_hot, axis=0) * one_hot, axis=1)) - 1

def reference(tokens, norm_gain, router_weight, expert_ids, gate_proj, up_proj, down_proj, value_weight, value_target, recency):
    wide = tokens.astype(jnp.float32)
    inverse = lax.rsqrt(lax.optimization_barrier(jnp.mean(wide * wide, axis=1, keepdims=True)) + 1e-05)
    normed = (wide * inverse * norm_gain).astype(jnp.bfloat16)
    logits = jnp.dot(normed, router_weight, preferred_element_type=jnp.float32)
    columns = jnp.arange(EXPERTS, dtype=jnp.int32)[None, :]
    first = lax.optimization_barrier(jnp.sum(jnp.where(expert_ids[:, 0:1] == columns, logits, 0.0), axis=1))
    second = lax.optimization_barrier(jnp.sum(jnp.where(expert_ids[:, 1:2] == columns, logits, 0.0), axis=1))
    gate_first = jax.nn.sigmoid(first - second)
    gate_second = jax.nn.sigmoid(second - first)
    grouped = expert_ids.reshape(N_EXPERT, 2 * TOK_DEV)
    ranks = jax.vmap(block_ranks)(grouped)
    per_expert = N_EXPERT * CAP
    block_index = jnp.arange(N_EXPERT, dtype=jnp.int32)[:, None]
    slot_global = (grouped * per_expert + block_index * CAP + ranks).reshape(-1).astype(jnp.int32)
    row_index = (jnp.arange(2 * TOKENS, dtype=jnp.int32) // 2).astype(jnp.int32)
    table = jnp.full((EXPERTS * per_expert,), TOKENS, dtype=jnp.int32).at[slot_global].set(row_index)
    padded = jnp.concatenate([normed, jnp.zeros((1, D), jnp.bfloat16)], axis=0)

    def one_expert(operands):
        indices, gate_mat, up_mat, down_mat = operands
        gathered = padded[indices]
        gate_part = jnp.dot(gathered, gate_mat, preferred_element_type=jnp.float32)
        up_part = jnp.dot(gathered, up_mat, preferred_element_type=jnp.float32)
        hidden = (jax.nn.silu(gate_part) * up_part).astype(jnp.bfloat16)
        return jnp.dot(hidden, down_mat, preferred_element_type=jnp.float32).astype(jnp.bfloat16)
    produced = lax.map(one_expert, (table.reshape(EXPERTS, per_expert), gate_proj, up_proj, down_proj))
    flat_out = produced.reshape(EXPERTS * per_expert, D)
    picked = flat_out[slot_global].reshape(TOKENS, 2, D)
    mixed = (wide + gate_first[:, None] * picked[:, 0].astype(jnp.float32) + gate_second[:, None] * picked[:, 1].astype(jnp.float32)).astype(jnp.bfloat16)
    values = jnp.tanh(jnp.dot(mixed, value_weight, preferred_element_type=jnp.float32))
    error = values - value_target.astype(jnp.float32)
    loss = jnp.sum(recency * error * error) / jnp.sum(recency)
    return (mixed, values, loss)
```

```python
import jax
import jax.numpy as jnp
from jax import lax
from jax.experimental import pallas as pl
from jax.experimental.pallas import tpu as pltpu
from jax.sharding import Mesh
from jax.sharding import PartitionSpec as P

EXPERT = ("expert_0", "expert_1", "expert_2", "expert_3")
F32 = jnp.float32
BF16 = jnp.bfloat16
I32 = jnp.int32
LANES = 128
SLOTS = 3
ROWS = 16


def vmem():
    return pl.BlockSpec(memory_space=pltpu.VMEM)


def smem():
    return pl.BlockSpec(memory_space=pltpu.SMEM)


def to_row(column):
    count = column.shape[0]
    at_row = lax.broadcasted_iota(I32, (count, count), 0)
    at_lane = lax.broadcasted_iota(I32, (count, count), 1)
    spread = jnp.where(at_row == at_lane, column, jnp.zeros_like(column))
    return jnp.sum(spread, axis=0, keepdims=True)


def route_kernel(tok_ref, gain_ref, router_ref, ids_ref, *refs):
    out_ref, gates_ref, where_ref, normed_ref, tall_ref, index_ref, index_smem, sem = refs
    count, width = tok_ref.shape
    parts = width // LANES
    experts = router_ref.shape[1]
    gain = gain_ref[...]

    def norm_rows(step, carry):
        start = pl.multiple_of(step * ROWS, ROWS)
        wide = tok_ref[pl.ds(start, ROWS), :].astype(F32)
        inverse = lax.rsqrt(jnp.mean(wide * wide, axis=1, keepdims=True) + 1e-05)
        normed = (wide * inverse * gain).astype(BF16)
        normed_ref[pl.ds(start, ROWS), :] = normed
        tall = normed.astype(F32).reshape(ROWS, parts, LANES)
        tall_ref[pl.ds(start, ROWS)] = tall.astype(BF16)
        return carry

    lax.fori_loop(0, count // ROWS, norm_rows, 0)
    tall_ref[count] = jnp.zeros((parts, LANES), BF16)

    ids = ids_ref[...]
    id_rows = [to_row(ids[:, k:k + 1]) for k in range(2)]
    expert_at = lax.broadcasted_iota(I32, (experts, count), 0)
    token_at = lax.broadcasted_iota(I32, (experts, count), 1)
    hits = [expert_at == row for row in id_rows]
    named = jnp.where(hits[0] | hits[1], 1.0, 0.0)
    before = jnp.where(
        lax.broadcasted_iota(I32, (count, count), 0) < lax.broadcasted_iota(I32, (count, count), 1), 1.0, 0.0
    )
    rank = jnp.dot(named.astype(BF16), before.astype(BF16), preferred_element_type=F32)
    rank = rank.astype(I32)
    for k in range(2):
        slot_of = jnp.sum(jnp.where(hits[k], rank, 0), axis=0, keepdims=True)
        where_ref[k:k + 1, :] = id_rows[k] * SLOTS + slot_of
    where_ref[2:, :] = jnp.zeros((where_ref.shape[0] - 2, count), I32)
    index_ref[...] = jnp.full(index_ref.shape, count, I32)
    for s in range(SLOTS):
        chosen = (hits[0] | hits[1]) & (rank == s)
        source = jnp.sum(jnp.where(chosen, token_at - count, 0), axis=1, keepdims=True) + count
        index_ref[s:s + 1, :] = to_row(source)
    copy = pltpu.make_async_copy(index_ref, index_smem, sem)
    copy.start()

    logits = jnp.dot(normed_ref[...], router_ref[...], preferred_element_type=F32)
    logits = jnp.transpose(logits)
    scores = [jnp.sum(jnp.where(hit, logits, 0.0), axis=0, keepdims=True) for hit in hits]
    gates_ref[0:1, :] = jax.nn.sigmoid(scores[0] - scores[1])
    gates_ref[1:2, :] = jax.nn.sigmoid(scores[1] - scores[0])
    gates_ref[2:, :] = jnp.zeros((gates_ref.shape[0] - 2, count), F32)
    copy.wait()

    for s in range(SLOTS):
        def send(step, carry, s=s):
            for i in range(8):
                e = step * 8 + i
                out_ref[e, s * parts:(s + 1) * parts] = tall_ref[index_smem[s, e]]
            return carry

        lax.fori_loop(0, experts // 8, send, 0)


def route(tokens, norm_gain, router_weight, expert_ids):
    count, width = tokens.shape
    experts = router_weight.shape[1]
    parts = width // LANES
    return pl.pallas_call(
        route_kernel,
        in_specs=[vmem()] * 4,
        out_specs=[vmem()] * 3,
        out_shape=[
            jax.ShapeDtypeStruct((experts, SLOTS * parts, LANES), BF16),
            jax.ShapeDtypeStruct((8, count), F32),
            jax.ShapeDtypeStruct((8, count), I32),
        ],
        scratch_shapes=[
            pltpu.VMEM((count, width), BF16),
            pltpu.VMEM((count + 1, parts, LANES), BF16),
            pltpu.VMEM((8, experts), I32),
            pltpu.SMEM((8, experts), I32),
            pltpu.SemaphoreType.DMA(()),
        ],
        name="route",
    )(tokens, norm_gain.reshape(1, width), router_weight, expert_ids)


def ffn_kernel(in_ref, gate_ref, up_ref, down_ref, out_ref, wide_ref, sum_ref):
    sources = in_ref.shape[0]
    width = wide_ref.shape[1]
    parts = width // LANES
    step = pl.program_id(0)

    @pl.when(step == 0)
    def _():
        for s in range(SLOTS):
            def widen(i, carry, s=s):
                start = pl.multiple_of(i * ROWS, ROWS)
                tall = in_ref[pl.ds(start, ROWS), s * parts:(s + 1) * parts].astype(F32)
                wide_ref[pl.ds(s * sources + start, ROWS), :] = tall.reshape(ROWS, width).astype(BF16)
                return carry

            lax.fori_loop(0, sources // ROWS, widen, 0)

    x = wide_ref[...]
    gate = jnp.dot(x, gate_ref[0], preferred_element_type=F32)
    up = jnp.dot(x, up_ref[0], preferred_element_type=F32)
    hidden = (jax.nn.silu(gate) * up).astype(BF16)
    part = jnp.dot(hidden, down_ref[0], preferred_element_type=F32)

    @pl.when(step == 0)
    def _():
        sum_ref[...] = part

    @pl.when(step > 0)
    def _():
        sum_ref[...] += part

    @pl.when(step == pl.num_programs(0) - 1)
    def _():
        for s in range(SLOTS):
            def heighten(i, carry, s=s):
                start = pl.multiple_of(i * ROWS, ROWS)
                wide = sum_ref[pl.ds(s * sources + start, ROWS), :]
                tall = wide.reshape(ROWS, parts, LANES).astype(BF16)
                out_ref[pl.ds(start, ROWS), s * parts:(s + 1) * parts] = tall
                return carry

            lax.fori_loop(0, sources // ROWS, heighten, 0)


def expert_ffn(received, gate_proj, up_proj, down_proj):
    sources = received.shape[0]
    _, width, hidden = gate_proj.shape
    tile = 256
    rows = SLOTS * sources
    return pl.pallas_call(
        ffn_kernel,
        grid=(hidden // tile,),
        in_specs=[
            vmem(),
            pl.BlockSpec((1, width, tile), lambda i: (0, 0, i)),
            pl.BlockSpec((1, width, tile), lambda i: (0, 0, i)),
            pl.BlockSpec((1, tile, width), lambda i: (0, i, 0)),
        ],
        out_specs=vmem(),
        out_shape=jax.ShapeDtypeStruct(received.shape, BF16),
        scratch_shapes=[pltpu.VMEM((rows, width), BF16), pltpu.VMEM((rows, width), F32)],
        compiler_params=pltpu.CompilerParams(vmem_limit_bytes=56 * 1024 * 1024),
        name="ffn",
    )(received, gate_proj, up_proj, down_proj)


def mix_kernel(
    tok_ref, back_ref, gates_ref, where_ref, weight_ref, target_ref, recency_ref,
    mixed_ref, values_ref, parts_ref, sum_ref,
):
    count, width = tok_ref.shape
    parts = width // LANES
    weight = weight_ref[...].astype(F32)

    def mix_rows(step, carry):
        start = pl.multiple_of(step * ROWS, ROWS)
        for i in range(ROWS):
            t = start + i
            total = None
            for k in range(2):
                at = where_ref[k, t]
                row = back_ref[at].astype(F32) * gates_ref[k, t]
                total = row if total is None else total + row
            sum_ref[i] = total
        update = sum_ref[...].reshape(ROWS, width)
        mixed = (tok_ref[pl.ds(start, ROWS), :].astype(F32) + update).astype(BF16)
        mixed_ref[pl.ds(start, ROWS), :] = mixed
        return carry

    lax.fori_loop(0, count // ROWS, mix_rows, 0)

    products = mixed_ref[...].astype(F32) * weight
    values = jnp.tanh(to_row(jnp.sum(products, axis=1, keepdims=True)))
    values_ref[...] = values
    error = values - target_ref[...].astype(F32)
    recency = recency_ref[...]
    weighted = jnp.sum(recency * error * error, axis=1, keepdims=True)
    total = jnp.sum(recency, axis=1, keepdims=True)
    lane = lax.broadcasted_iota(I32, parts_ref.shape, 1)
    parts_ref[...] = jnp.where(lane == 0, weighted, jnp.where(lane == 1, total, 0.0))


def mix(tokens, back, gates, where, value_weight, value_target, recency, devices):
    count, width = tokens.shape
    parts = width // LANES
    return pl.pallas_call(
        mix_kernel,
        in_specs=[vmem()] * 2 + [smem()] * 2 + [vmem()] * 3,
        out_specs=[vmem()] * 3,
        out_shape=[
            jax.ShapeDtypeStruct((count, width), BF16),
            jax.ShapeDtypeStruct((1, count), F32),
            jax.ShapeDtypeStruct((devices, LANES), F32),
        ],
        scratch_shapes=[pltpu.VMEM((ROWS, parts, LANES), F32)],
        name="mix",
    )(
        tokens, back.reshape(devices * SLOTS, parts, LANES), gates, where, value_weight.reshape(1, width),
        value_target.reshape(1, count), recency.reshape(1, count),
    )


def exchange(x):
    return lax.all_to_all(x, EXPERT, split_axis=0, concat_axis=0, tiled=True)


def body(
    tokens,
    norm_gain,
    router_weight,
    expert_ids,
    gate_proj,
    up_proj,
    down_proj,
    value_weight,
    value_target,
    recency,
):
    count, width = tokens.shape
    experts = router_weight.shape[1]
    outgoing, gates, where = route(tokens, norm_gain, router_weight, expert_ids)
    produced = expert_ffn(exchange(outgoing), gate_proj, up_proj, down_proj)
    back = exchange(produced)
    mixed, values, sums = mix(
        tokens, back, gates, where, value_weight, value_target, recency, experts
    )
    everyone = exchange(sums.reshape(experts, 1, LANES)).reshape(experts, LANES)
    total = jnp.sum(everyone, axis=0)
    return (mixed, values.reshape(count), total[0] / total[1])


def solution(mesh):
    finer = Mesh(mesh.devices.reshape(4, 4, 4, 2), EXPERT)
    in_specs = (
        P(EXPERT, None),
        P(),
        P(),
        P(EXPERT, None),
        P(EXPERT, None, None),
        P(EXPERT, None, None),
        P(EXPERT, None, None),
        P(),
        P(EXPERT),
        P(EXPERT),
    )
    out_specs = (P(EXPERT, None), P(EXPERT), P())
    return jax.shard_map(body, mesh=finer, in_specs=in_specs, out_specs=out_specs, check_vma=False)
```

```python
import jax
import jax.numpy as jnp
from jax import lax
from jax.experimental import pallas as pl
from jax.experimental.pallas import tpu as pltpu
from jax.sharding import Mesh
from jax.sharding import PartitionSpec as P

EXPERT = ("expert_0", "expert_1", "expert_2", "expert_3")
F32 = jnp.float32
BF16 = jnp.bfloat16
I32 = jnp.int32
LANES = 128
SLOTS = 3
ROWS = 16
CHUNKS = 4
MIB = 1024 * 1024
NEAR = pl.BlockSpec(memory_space=pltpu.VMEM)
SCALARS = pl.BlockSpec(memory_space=pltpu.SMEM)
FAR = pl.BlockSpec(memory_space=pltpu.HBM)


def params(mib):
    return pltpu.CompilerParams(vmem_limit_bytes=mib * MIB)


def cost(flops, moved):
    return pl.CostEstimate(flops=flops, transcendentals=0, bytes_accessed=moved)


def kept(x):
    return pltpu.with_memory_space_constraint(x, pltpu.VMEM)


def far(x):
    return pltpu.with_memory_space_constraint(x, pltpu.HBM)


def start_all(pairs, sems):
    copies = [pltpu.make_async_copy(src, dst, sems.at[i]) for i, (src, dst) in enumerate(pairs)]
    for copy in copies:
        copy.start()
    return copies


def pieces_of(count, pieces):
    size = count // pieces
    return [pl.ds(i * size, size) for i in range(pieces)]


def iota(shape, dim):
    return lax.broadcasted_iota(I32, shape, dim)


def to_row(column):
    count = column.shape[0]
    spread = jnp.where(iota((count, count), 0) == iota((count, count), 1), column, jnp.zeros_like(column))
    return jnp.sum(spread, axis=0, keepdims=True)


def slots_of(ids_ref, experts):
    count = ids_ref.shape[1]
    hits = [iota((experts, count), 0) == ids_ref[k:k + 1, :] for k in range(2)]
    named = jnp.where(hits[0] | hits[1], 1.0, 0.0).astype(BF16)
    before = jnp.where(iota((count, count), 0) < iota((count, count), 1), 1.0, 0.0).astype(BF16)
    rank = jnp.dot(named, before, preferred_element_type=F32)
    return hits, rank


def norm(wide, gain):
    inverse = lax.rsqrt(jnp.mean(wide * wide, axis=1, keepdims=True) + 1e-05)
    return (wide * inverse * gain).astype(BF16)


def route_kernel(
    tok_ref, gain_ref, ids_ref, out_ref,
    near_ref, gain_near, ids_near, tall_ref, piece_ref, index_ref, index_smem, sems, out_sems, index_sem,
):
    count, width = tok_ref.shape
    parts = width // LANES
    experts = out_ref.shape[0]
    copies = start_all(
        [(ids_ref, ids_near), (gain_ref, gain_near)]
        + [(tok_ref.at[rows], near_ref.at[rows]) for rows in pieces_of(count, CHUNKS)],
        sems,
    )
    copies[0].wait()
    hits, rank = slots_of(ids_near, experts)
    named = hits[0] | hits[1]
    token = (iota((8, count), 1) - count).astype(F32).astype(BF16)
    for s in range(SLOTS):
        chosen = jnp.where(named & (rank == s), 1.0, 0.0).astype(BF16)
        source = lax.dot_general(token, chosen, (((1,), (1,)), ((), ())), preferred_element_type=F32)
        index_ref[s:s + 1, :] = source[0:1].astype(I32) + count
    index_ref[SLOTS:, :] = jnp.zeros((8 - SLOTS, experts), I32)
    index_copy = pltpu.make_async_copy(index_ref, index_smem, index_sem)
    index_copy.start()
    tall_ref[count] = jnp.zeros((parts, LANES), BF16)
    copies[1].wait()
    gain = gain_near[...]
    chunk = count // CHUNKS
    for c in range(CHUNKS):
        copies[2 + c].wait()

        def norm_rows(step, carry, c=c):
            start = pl.multiple_of(c * chunk + step * ROWS, ROWS)
            normed = norm(near_ref[pl.ds(start, ROWS), :].astype(F32), gain)
            tall_ref[pl.ds(start, ROWS)] = normed.astype(F32).reshape(ROWS, parts, LANES).astype(BF16)
            return carry

        lax.fori_loop(0, chunk // ROWS, norm_rows, 0)
    index_copy.wait()
    chunk = experts // CHUNKS
    sent = []
    for c, rows in enumerate(pieces_of(experts, CHUNKS)):
        def send(step, carry, c=c):
            for i in range(4):
                e = c * chunk + step * 4 + i
                for s in range(SLOTS):
                    piece_ref[e, s * parts:(s + 1) * parts] = tall_ref[index_smem[s, e]]
            return carry

        lax.fori_loop(0, chunk // 4, send, 0)
        sent.append(pltpu.make_async_copy(piece_ref.at[rows], out_ref.at[rows], out_sems.at[c]))
        sent[c].start()
    for copy in sent:
        copy.wait()


def route(tokens, norm_gain, ids, experts):
    count, width = tokens.shape
    parts = width // LANES
    pieces = (experts, SLOTS * parts, LANES)
    return pl.pallas_call(
        route_kernel,
        in_specs=[FAR] * 3,
        out_specs=FAR,
        out_shape=pltpu.HBM(pieces, BF16),
        scratch_shapes=[
            pltpu.VMEM((count, width), BF16),
            pltpu.VMEM(norm_gain.shape, F32),
            pltpu.VMEM(ids.shape, I32),
            pltpu.VMEM((count + 1, parts, LANES), BF16),
            pltpu.VMEM(pieces, BF16),
            pltpu.VMEM((8, experts), I32),
            pltpu.SMEM((8, experts), I32),
            pltpu.SemaphoreType.DMA((2 + CHUNKS,)),
            pltpu.SemaphoreType.DMA((CHUNKS,)),
            pltpu.SemaphoreType.DMA(()),
        ],
        compiler_params=params(16),
        name="route",
    )(far(tokens), far(norm_gain), far(ids))


def gate_kernel(tok_ref, gain_ref, router_ref, ids_ref, gates_ref, where_ref, tall_ref, normed_ref):
    count, width = tok_ref.shape
    parts = width // LANES
    experts = router_ref.shape[1]
    gain = gain_ref[...]

    def norm_rows(step, carry):
        start = pl.multiple_of(step * ROWS, ROWS)
        wide = tok_ref[pl.ds(start, ROWS), :].astype(F32)
        normed_ref[pl.ds(start, ROWS), :] = norm(wide, gain)
        tall_ref[pl.ds(start, ROWS)] = wide.reshape(ROWS, parts, LANES).astype(BF16)
        return carry

    lax.fori_loop(0, count // ROWS, norm_rows, 0)
    hits, rank = slots_of(ids_ref, experts)
    logits = jnp.transpose(jnp.dot(normed_ref[...], router_ref[...], preferred_element_type=F32))
    scores = []
    where_ref[...] = jnp.zeros(where_ref.shape, I32)
    gates_ref[...] = jnp.zeros(gates_ref.shape, F32)
    for k in range(2):
        slot = jnp.sum(jnp.where(hits[k], rank, 0.0), axis=0, keepdims=True).astype(I32)
        where_ref[k:k + 1, :] = ids_ref[k:k + 1, :] * SLOTS + slot
        scores.append(jnp.sum(jnp.where(hits[k], logits, 0.0), axis=0, keepdims=True))
    gates_ref[0:1, :] = jax.nn.sigmoid(scores[0] - scores[1])
    gates_ref[1:2, :] = jax.nn.sigmoid(scores[1] - scores[0])


def gate(tokens, norm_gain, router_weight, ids):
    count, width = tokens.shape
    parts = width // LANES
    return pl.pallas_call(
        gate_kernel,
        in_specs=[NEAR] * 4,
        out_specs=[NEAR] * 3,
        out_shape=[
            jax.ShapeDtypeStruct((8, count), F32),
            jax.ShapeDtypeStruct((8, count), I32),
            pltpu.HBM((count, parts, LANES), BF16),
        ],
        scratch_shapes=[pltpu.VMEM((count, width), BF16)],
        compiler_params=params(16),
        cost_estimate=cost(10**10, 4 * MIB),
        name="gate",
    )(tokens, norm_gain, router_weight, ids)


def ffn_kernel(
    in_ref, gate_ref, up_ref, down_ref, out_ref,
    gate_near, up_near, down_near, wide_ref, hidden_ref, tall_ref, sems, out_sems,
):
    rows, parts, _ = in_ref.shape
    width, hidden = gate_near.shape
    tiles = [slice(start, start + 256) for start in range(0, hidden, 256)]
    pairs = []
    for tile in tiles:
        pairs.append((gate_ref.at[0, :, tile], gate_near.at[:, tile]))
        pairs.append((up_ref.at[0, :, tile], up_near.at[:, tile]))
    for tile in tiles:
        pairs.append((down_ref.at[0, tile, :], down_near.at[tile, :]))
    copies = start_all(pairs, sems)

    def widen(i, carry):
        start = pl.multiple_of(i * ROWS, ROWS)
        tall = in_ref[pl.ds(start, ROWS)].astype(F32)
        wide_ref[pl.ds(start, ROWS), :] = tall.reshape(ROWS, width).astype(BF16)
        return carry

    lax.fori_loop(0, rows // ROWS, widen, 0)
    for i, tile in enumerate(tiles):
        copies[2 * i].wait()
        copies[2 * i + 1].wait()
        x = wide_ref[...]
        gated = jnp.dot(x, gate_near[:, tile], preferred_element_type=F32)
        upped = jnp.dot(x, up_near[:, tile], preferred_element_type=F32)
        hidden_ref[:, tile] = (jax.nn.silu(gated) * upped).astype(BF16)
    for i in range(len(tiles)):
        copies[2 * len(tiles) + i].wait()
    for start in range(0, width, 512):
        tile = slice(start, start + 512)
        wide_ref[:, tile] = jnp.dot(hidden_ref[...], down_near[:, tile], preferred_element_type=F32).astype(BF16)
    pieces = out_sems.shape[0]
    sent = []
    for p, piece in enumerate(pieces_of(rows, pieces)):
        def heighten(i, carry, p=p):
            start = pl.multiple_of(p * (rows // pieces) + i * ROWS, ROWS)
            wide = wide_ref[pl.ds(start, ROWS), :].astype(F32)
            tall_ref[pl.ds(start, ROWS)] = wide.reshape(ROWS, parts, LANES).astype(BF16)
            return carry

        lax.fori_loop(0, rows // pieces // ROWS, heighten, 0)
        sent.append(pltpu.make_async_copy(tall_ref.at[piece], out_ref.at[piece], out_sems.at[p]))
        sent[p].start()
    for copy in sent:
        copy.wait()


def expert_ffn(received, gate_proj, up_proj, down_proj):
    rows, parts, _ = received.shape
    _, width, hidden = gate_proj.shape
    return pl.pallas_call(
        ffn_kernel,
        in_specs=[NEAR] + [FAR] * 3,
        out_specs=FAR,
        out_shape=pltpu.HBM(received.shape, BF16),
        scratch_shapes=[
            pltpu.VMEM((width, hidden), BF16),
            pltpu.VMEM((width, hidden), BF16),
            pltpu.VMEM((hidden, width), BF16),
            pltpu.VMEM((rows, width), BF16),
            pltpu.VMEM((rows, hidden), BF16),
            pltpu.VMEM((rows, parts, LANES), BF16),
            pltpu.SemaphoreType.DMA((3 * (hidden // 256),)),
            pltpu.SemaphoreType.DMA((6,)),
        ],
        compiler_params=params(40),
        cost_estimate=cost(6 * rows * width * hidden, 24 * MIB),
        name="ffn",
    )(kept(received), far(gate_proj), far(up_proj), far(down_proj))


def mix_kernel(
    back_ref, token_ref, gates_ref, where_ref, weight_ref, target_ref, recency_ref,
    mixed_ref, values_ref, sums_ref,
    tall_ref, near_ref, score_ref, sems, out_sems,
):
    count, parts, _ = token_ref.shape
    rows = pieces_of(count, CHUNKS)
    copies = start_all([(token_ref.at[r], tall_ref.at[r]) for r in rows], sems)
    weight = weight_ref[...]
    chunk = count // CHUNKS
    sent = []
    for c in range(CHUNKS):
        copies[c].wait()

        def mix_rows(step, carry, c=c):
            for i in range(8):
                t = c * chunk + step * 8 + i
                total = tall_ref[t].astype(F32)
                for k in range(2):
                    total = total + gates_ref[k, t] * back_ref[where_ref[k, t]].astype(F32)
                mixed = total.astype(BF16)
                near_ref[t] = mixed
                scored = mixed.astype(F32) * weight
                score_ref[t] = jnp.sum(scored.reshape(parts // 8, 8, LANES), axis=0)
            return carry

        lax.fori_loop(0, chunk // 8, mix_rows, 0)
        sent.append(pltpu.make_async_copy(near_ref.at[rows[c]], mixed_ref.at[rows[c]], out_sems.at[c]))
        sent[c].start()
    by_lane = jnp.sum(score_ref[...], axis=1)
    values = jnp.tanh(to_row(jnp.sum(by_lane, axis=1, keepdims=True)))
    values_ref[...] = values
    error = values - target_ref[...].astype(F32)
    recency = recency_ref[...]
    weighted = jnp.sum(recency * error * error, axis=1, keepdims=True)
    total = jnp.sum(recency, axis=1, keepdims=True)
    lane = iota(sums_ref.shape, 1)
    sums_ref[...] = jnp.where(lane == 0, weighted, jnp.where(lane == 1, total, 0.0))
    for copy in sent:
        copy.wait()


def mix(back, tall, gates, where, weight, target, recency, devices):
    count, parts, _ = tall.shape
    return pl.pallas_call(
        mix_kernel,
        in_specs=[NEAR, FAR] + [SCALARS] * 2 + [NEAR] * 3,
        out_specs=[FAR] + [NEAR] * 2,
        out_shape=[
            pltpu.HBM(tall.shape, BF16),
            jax.ShapeDtypeStruct((1, count), F32),
            jax.ShapeDtypeStruct((devices, LANES), F32),
        ],
        scratch_shapes=[
            pltpu.VMEM((count, parts, LANES), BF16),
            pltpu.VMEM((count, parts, LANES), BF16),
            pltpu.VMEM((count, 8, LANES), F32),
            pltpu.SemaphoreType.DMA((CHUNKS,)),
            pltpu.SemaphoreType.DMA((CHUNKS,)),
        ],
        compiler_params=params(16),
        name="mix",
    )(kept(back), far(tall), gates, where, weight, target, recency)


def widen_kernel(tall_ref, out_ref):
    count, width = out_ref.shape

    def widen(i, carry):
        start = pl.multiple_of(i * ROWS, ROWS)
        tall = tall_ref[pl.ds(start, ROWS)].astype(F32)
        out_ref[pl.ds(start, ROWS), :] = tall.reshape(ROWS, width).astype(BF16)
        return carry

    lax.fori_loop(0, count // ROWS, widen, 0)


def widen_rows(tall):
    count, parts, _ = tall.shape
    return pl.pallas_call(
        widen_kernel,
        in_specs=[NEAR],
        out_specs=NEAR,
        out_shape=jax.ShapeDtypeStruct((count, parts * LANES), BF16),
        compiler_params=params(8),
        cost_estimate=cost(10**10, 2 * MIB),
        name="widen",
    )(far(tall))


def exchange(x):
    return lax.all_to_all(x, EXPERT, split_axis=0, concat_axis=0, tiled=True)


def body(
    tokens,
    norm_gain,
    router_weight,
    expert_ids,
    gate_proj,
    up_proj,
    down_proj,
    value_weight,
    value_target,
    recency,
):
    count, width = tokens.shape
    experts = router_weight.shape[1]
    parts = width // LANES
    pieces = (experts, SLOTS * parts, LANES)
    rows = (experts * SLOTS, parts, LANES)
    ids = expert_ids.T
    gain = norm_gain.reshape(1, width)
    received = exchange(route(tokens, gain, ids, experts))
    gates, where, tall = gate(tokens, gain, router_weight, ids)
    produced = expert_ffn(received.reshape(rows), gate_proj, up_proj, down_proj)
    back = exchange(produced.reshape(pieces))
    mixed, values, sums = mix(
        back.reshape(rows), tall, gates, where, value_weight.reshape(parts, LANES).astype(F32),
        value_target.reshape(1, count), recency.reshape(1, count), experts,
    )
    everyone = exchange(sums.reshape(experts, 1, LANES)).reshape(experts, LANES)
    total = jnp.sum(everyone, axis=0)
    return (widen_rows(mixed), values.reshape(count), total[0] / total[1])


def solution(mesh):
    finer = Mesh(mesh.devices.reshape(4, 4, 4, 2), EXPERT)
    in_specs = (
        P(EXPERT, None),
        P(),
        P(),
        P(EXPERT, None),
        P(EXPERT, None, None),
        P(EXPERT, None, None),
        P(EXPERT, None, None),
        P(),
        P(EXPERT),
        P(EXPERT),
    )
    out_specs = (P(EXPERT, None), P(EXPERT), P())
    return jax.shard_map(body, mesh=finer, in_specs=in_specs, out_specs=out_specs, check_vma=False)
```

```python
import jax
import jax.numpy as jnp
from jax import lax
from jax.experimental import pallas as pl
from jax.experimental.pallas import tpu as pltpu
from jax.sharding import Mesh
from jax.sharding import PartitionSpec as P

EXPERT = ("expert_0", "expert_1", "expert_2", "expert_3")
F32 = jnp.float32
BF16 = jnp.bfloat16
I32 = jnp.int32
LANES = 128
SLOTS = 3
ROWS = 16
CHUNKS = 4
MIB = 1024 * 1024
NEAR = pl.BlockSpec(memory_space=pltpu.VMEM)
SCALARS = pl.BlockSpec(memory_space=pltpu.SMEM)
FAR = pl.BlockSpec(memory_space=pltpu.HBM)


def params(mib):
    return pltpu.CompilerParams(vmem_limit_bytes=mib * MIB)


def cost(flops, moved):
    return pl.CostEstimate(flops=flops, transcendentals=0, bytes_accessed=moved)


def kept(x):
    return pltpu.with_memory_space_constraint(x, pltpu.VMEM)


def far(x):
    return pltpu.with_memory_space_constraint(x, pltpu.HBM)


def start_all(pairs, sems):
    copies = [pltpu.make_async_copy(src, dst, sems.at[i]) for i, (src, dst) in enumerate(pairs)]
    for copy in copies:
        copy.start()
    return copies


def pieces_of(count, pieces):
    size = count // pieces
    return [pl.ds(i * size, size) for i in range(pieces)]


def iota(shape, dim):
    return lax.broadcasted_iota(I32, shape, dim)


def to_row(column):
    count = column.shape[0]
    spread = jnp.where(iota((count, count), 0) == iota((count, count), 1), column, jnp.zeros_like(column))
    return jnp.sum(spread, axis=0, keepdims=True)


def slots_of(ids_ref, experts):
    count = ids_ref.shape[1]
    hits = [iota((experts, count), 0) == ids_ref[k:k + 1, :] for k in range(2)]
    named = jnp.where(hits[0] | hits[1], 1.0, 0.0).astype(BF16)
    before = jnp.where(iota((count, count), 0) < iota((count, count), 1), 1.0, 0.0).astype(BF16)
    rank = jnp.dot(named, before, preferred_element_type=F32)
    return hits, rank


def norm(wide, gain):
    inverse = lax.rsqrt(jnp.mean(wide * wide, axis=1, keepdims=True) + 1e-05)
    return (wide * inverse * gain).astype(BF16)


def route_kernel(
    tok_ref, gain_ref, ids_ref, out_ref,
    near_ref, gain_near, ids_near, tall_ref, piece_ref, index_ref, index_smem, sems, out_sems, index_sem,
):
    count, width = tok_ref.shape
    parts = width // LANES
    experts = out_ref.shape[0]
    copies = start_all(
        [(ids_ref, ids_near), (gain_ref, gain_near)]
        + [(tok_ref.at[rows], near_ref.at[rows]) for rows in pieces_of(count, CHUNKS)],
        sems,
    )
    copies[0].wait()
    hits, rank = slots_of(ids_near, experts)
    named = hits[0] | hits[1]
    token = (iota((8, count), 1) - count).astype(F32).astype(BF16)
    for s in range(SLOTS):
        chosen = jnp.where(named & (rank == s), 1.0, 0.0).astype(BF16)
        source = lax.dot_general(token, chosen, (((1,), (1,)), ((), ())), preferred_element_type=F32)
        index_ref[s:s + 1, :] = source[0:1].astype(I32) + count
    index_ref[SLOTS:, :] = jnp.zeros((8 - SLOTS, experts), I32)
    index_copy = pltpu.make_async_copy(index_ref, index_smem, index_sem)
    index_copy.start()
    tall_ref[count] = jnp.zeros((parts, LANES), BF16)
    copies[1].wait()
    gain = gain_near[...]
    chunk = count // CHUNKS
    for c in range(CHUNKS):
        copies[2 + c].wait()

        def norm_rows(step, carry, c=c):
            start = pl.multiple_of(c * chunk + step * ROWS, ROWS)
            normed = norm(near_ref[pl.ds(start, ROWS), :].astype(F32), gain)
            tall_ref[pl.ds(start, ROWS)] = normed.astype(F32).reshape(ROWS, parts, LANES).astype(BF16)
            return carry

        lax.fori_loop(0, chunk // ROWS, norm_rows, 0)
    index_copy.wait()
    chunk = experts // CHUNKS
    sent = []
    for c, rows in enumerate(pieces_of(experts, CHUNKS)):
        def send(step, carry, c=c):
            for i in range(4):
                e = c * chunk + step * 4 + i
                for s in range(SLOTS):
                    piece_ref[e, s * parts:(s + 1) * parts] = tall_ref[index_smem[s, e]]
            return carry

        lax.fori_loop(0, chunk // 4, send, 0)
        sent.append(pltpu.make_async_copy(piece_ref.at[rows], out_ref.at[rows], out_sems.at[c]))
        sent[c].start()
    for copy in sent:
        copy.wait()


def route(tokens, norm_gain, ids, experts):
    count, width = tokens.shape
    parts = width // LANES
    pieces = (experts, SLOTS * parts, LANES)
    return pl.pallas_call(
        route_kernel,
        in_specs=[FAR] * 3,
        out_specs=FAR,
        out_shape=pltpu.HBM(pieces, BF16),
        scratch_shapes=[
            pltpu.VMEM((count, width), BF16),
            pltpu.VMEM(norm_gain.shape, F32),
            pltpu.VMEM(ids.shape, I32),
            pltpu.VMEM((count + 1, parts, LANES), BF16),
            pltpu.VMEM(pieces, BF16),
            pltpu.VMEM((8, experts), I32),
            pltpu.SMEM((8, experts), I32),
            pltpu.SemaphoreType.DMA((2 + CHUNKS,)),
            pltpu.SemaphoreType.DMA((CHUNKS,)),
            pltpu.SemaphoreType.DMA(()),
        ],
        compiler_params=params(16),
        name="route",
    )(far(tokens), far(norm_gain), far(ids))


def gate_kernel(
    *refs,
):
    inputs, (gates_ref, where_ref, base_ref, out_ref), scratch = refs[:6], refs[6:10], refs[10:]
    tok_ref, gain_ref, router_ref, ids_ref, weight_ref, down_ref, normed_ref, score_ref, sems = scratch
    for copy in start_all(zip(inputs, scratch[:6]), sems):
        copy.wait()
    count, width = tok_ref.shape
    experts = router_ref.shape[1]
    gain = gain_ref[...]
    weight = weight_ref[...]

    def norm_rows(step, carry):
        start = pl.multiple_of(step * ROWS, ROWS)
        wide = tok_ref[pl.ds(start, ROWS), :].astype(F32)
        normed_ref[pl.ds(start, ROWS), :] = norm(wide, gain)
        score_ref[pl.ds(start, ROWS), :] = jnp.sum(wide * weight, axis=1, keepdims=True)
        return carry

    lax.fori_loop(0, count // ROWS, norm_rows, 0)
    base_ref[...] = to_row(score_ref[...])
    hits, rank = slots_of(ids_ref, experts)
    logits = jnp.transpose(jnp.dot(normed_ref[...], router_ref[...], preferred_element_type=F32))
    scores = []
    where_ref[...] = jnp.zeros(where_ref.shape, I32)
    gates_ref[...] = jnp.zeros(gates_ref.shape, F32)
    for k in range(2):
        slot = jnp.sum(jnp.where(hits[k], rank, 0.0), axis=0, keepdims=True).astype(I32)
        where_ref[k:k + 1, :] = ids_ref[k:k + 1, :] * SLOTS + slot
        scores.append(jnp.sum(jnp.where(hits[k], logits, 0.0), axis=0, keepdims=True))
    gates_ref[0:1, :] = jax.nn.sigmoid(scores[0] - scores[1])
    gates_ref[1:2, :] = jax.nn.sigmoid(scores[1] - scores[0])

    def score_rows(step, carry):
        start = pl.multiple_of(step * ROWS, ROWS)
        products = down_ref[0, pl.ds(start, ROWS), :].astype(F32) * weight
        scored = jnp.broadcast_to(jnp.sum(products, axis=1, keepdims=True), (ROWS, LANES))
        high = scored.astype(BF16)
        out_ref[pl.ds(start, ROWS), 0:LANES] = high
        out_ref[pl.ds(start, ROWS), LANES:] = (scored - high.astype(F32)).astype(BF16)
        return carry

    lax.fori_loop(0, down_ref.shape[1] // ROWS, score_rows, 0)


def gate(tokens, norm_gain, router_weight, ids, weight, down_proj):
    count, width = tokens.shape
    inputs = (tokens, norm_gain, router_weight, ids, weight, down_proj)
    return pl.pallas_call(
        gate_kernel,
        in_specs=[FAR] * 6,
        out_specs=[NEAR] * 4,
        out_shape=[
            jax.ShapeDtypeStruct((8, count), F32),
            jax.ShapeDtypeStruct((8, count), I32),
            jax.ShapeDtypeStruct((1, count), F32),
            jax.ShapeDtypeStruct((down_proj.shape[1], 2 * LANES), BF16),
        ],
        scratch_shapes=[pltpu.VMEM(x.shape, x.dtype) for x in inputs]
        + [pltpu.VMEM((count, width), BF16), pltpu.VMEM((count, 1), F32), pltpu.SemaphoreType.DMA((6,))],
        compiler_params=params(24),
        cost_estimate=cost(10**10, 10 * MIB),
        name="gate",
    )(*[far(x) for x in inputs])


def up_kernel(
    in_ref, gate_ref, up_ref, score_ref, hidden_out, values_ref,
    gate_near, up_near, score_near, wide_ref, hidden_ref, sems, out_sem,
):
    sources = in_ref.shape[0]
    width, hidden = gate_near.shape
    parts = width // LANES
    tiles = [slice(start, start + 256) for start in range(0, hidden, 256)]
    pairs = []
    for tile in tiles:
        pairs.append((gate_ref.at[0, :, tile], gate_near.at[:, tile]))
        pairs.append((up_ref.at[0, :, tile], up_near.at[:, tile]))
    copies = start_all(pairs + [(score_ref, score_near)], sems)
    for s in range(SLOTS):
        def widen(i, carry, s=s):
            start = pl.multiple_of(i * ROWS, ROWS)
            tall = in_ref[pl.ds(start, ROWS), s * parts:(s + 1) * parts].astype(F32)
            wide_ref[pl.ds(s * sources + start, ROWS), :] = tall.reshape(ROWS, width).astype(BF16)
            return carry

        lax.fori_loop(0, sources // ROWS, widen, 0)
    for i, tile in enumerate(tiles):
        copies[2 * i].wait()
        copies[2 * i + 1].wait()
        x = wide_ref[...]
        gated = jnp.dot(x, gate_near[:, tile], preferred_element_type=F32)
        upped = jnp.dot(x, up_near[:, tile], preferred_element_type=F32)
        hidden_ref[:, tile] = (jax.nn.silu(gated) * upped).astype(BF16)
    sent = pltpu.make_async_copy(hidden_ref, hidden_out, out_sem)
    sent.start()
    copies[-1].wait()
    both = jnp.dot(hidden_ref[...], score_near[...], preferred_element_type=F32)
    both = both[:, :LANES] + both[:, LANES:]
    lane = iota((sources, LANES), 1)
    by_slot = jnp.zeros((sources, LANES), F32)
    for s in range(SLOTS):
        by_slot = jnp.where(lane == s, both[s * sources:(s + 1) * sources], by_slot)
    values_ref[...] = by_slot
    sent.wait()


def expert_up(received, gate_proj, up_proj, scores):
    sources = received.shape[0]
    rows = SLOTS * sources
    _, width, hidden = gate_proj.shape
    return pl.pallas_call(
        up_kernel,
        in_specs=[NEAR] + [FAR] * 3,
        out_specs=[FAR, NEAR],
        out_shape=[pltpu.HBM((rows, hidden), BF16), jax.ShapeDtypeStruct((sources, LANES), F32)],
        scratch_shapes=[
            pltpu.VMEM((width, hidden), BF16),
            pltpu.VMEM((width, hidden), BF16),
            pltpu.VMEM(scores.shape, BF16),
            pltpu.VMEM((rows, width), BF16),
            pltpu.VMEM((rows, hidden), BF16),
            pltpu.SemaphoreType.DMA((2 * (hidden // 256) + 1,)),
            pltpu.SemaphoreType.DMA(()),
        ],
        compiler_params=params(40),
        cost_estimate=cost(4 * rows * width * hidden, 18 * MIB),
        name="expert_up",
    )(kept(received), far(gate_proj), far(up_proj), far(scores))


def down_kernel(hidden_ref, down_ref, out_ref, hidden_near, down_near, wide_ref, piece_ref, sems, out_sems):
    hidden, width = down_near.shape
    sources = out_ref.shape[0]
    parts = width // LANES
    tiles = [slice(start, start + 1024) for start in range(0, width, 1024)]
    copies = start_all(
        [(hidden_ref, hidden_near)] + [(down_ref.at[0, :, tile], down_near.at[:, tile]) for tile in tiles], sems
    )
    copies[0].wait()
    for i, tile in enumerate(tiles):
        copies[1 + i].wait()
        for start in range(tile.start, tile.stop, 512):
            at = slice(start, start + 512)
            wide = jnp.dot(hidden_near[...], down_near[:, at], preferred_element_type=F32)
            wide_ref[:, at] = wide.astype(BF16)
    pieces = out_sems.shape[0]
    chunk = sources // pieces
    sent = []
    for p, piece in enumerate(pieces_of(sources, pieces)):
        for s in range(SLOTS):
            def heighten(i, carry, p=p, s=s):
                start = pl.multiple_of(p * chunk + i * ROWS, ROWS)
                wide = wide_ref[pl.ds(s * sources + start, ROWS), :].astype(F32)
                tall = wide.reshape(ROWS, parts, LANES).astype(BF16)
                piece_ref[pl.ds(start, ROWS), s * parts:(s + 1) * parts] = tall
                return carry

            lax.fori_loop(0, chunk // ROWS, heighten, 0)
        sent.append(pltpu.make_async_copy(piece_ref.at[piece], out_ref.at[piece], out_sems.at[p]))
        sent[p].start()
    for copy in sent:
        copy.wait()


def expert_down(hidden_rows, down_proj):
    rows, hidden = hidden_rows.shape
    width = down_proj.shape[2]
    shape = (rows // SLOTS, SLOTS * (width // LANES), LANES)
    return pl.pallas_call(
        down_kernel,
        in_specs=[FAR] * 2,
        out_specs=FAR,
        out_shape=pltpu.HBM(shape, BF16),
        scratch_shapes=[
            pltpu.VMEM((rows, hidden), BF16),
            pltpu.VMEM((hidden, width), BF16),
            pltpu.VMEM((rows, width), BF16),
            pltpu.VMEM(shape, BF16),
            pltpu.SemaphoreType.DMA((1 + width // 1024,)),
            pltpu.SemaphoreType.DMA((4,)),
        ],
        compiler_params=params(24),
        cost_estimate=cost(2 * rows * width * hidden, 12 * MIB),
        name="expert_down",
    )(far(hidden_rows), far(down_proj))


def value_kernel(part_ref, ids_ref, gates_ref, base_ref, target_ref, recency_ref, values_ref, sums_ref):
    experts = part_ref.shape[0]
    hits, rank = slots_of(ids_ref, experts)
    total = base_ref[...]
    part = jnp.zeros(rank.shape, F32)
    for s in range(SLOTS):
        part = jnp.where(rank == s, part_ref[:, s:s + 1], part)
    for k in range(2):
        picked = jnp.sum(jnp.where(hits[k], part, 0.0), axis=0, keepdims=True)
        total = total + gates_ref[k:k + 1, :] * picked
    values = jnp.tanh(total)
    values_ref[...] = values
    error = values - target_ref[...].astype(F32)
    recency = recency_ref[...]
    weighted = jnp.sum(recency * error * error, axis=1, keepdims=True)
    weights = jnp.sum(recency, axis=1, keepdims=True)
    lane = iota(sums_ref.shape, 1)
    sums_ref[...] = jnp.where(lane == 0, weighted, jnp.where(lane == 1, weights, 0.0))


def value(part, ids, gates, base, target, recency):
    return pl.pallas_call(
        value_kernel,
        in_specs=[NEAR] * 6,
        out_specs=[NEAR] * 2,
        out_shape=[jax.ShapeDtypeStruct(base.shape, F32), jax.ShapeDtypeStruct((1, LANES), F32)],
        compiler_params=params(8),
        cost_estimate=cost(10**9, MIB),
        name="value",
    )(part, ids, gates, base, target, recency)


def mix_kernel(
    back_ref, token_ref, gates_ref, where_ref, mixed_ref, near_ref, out_near, sum_ref, sems, out_sems
):
    count, width = token_ref.shape
    parts = width // LANES
    rows = pieces_of(count, CHUNKS)
    copies = start_all([(token_ref.at[r], near_ref.at[r]) for r in rows], sems)
    chunk = count // CHUNKS
    sent = []
    for c in range(CHUNKS):
        copies[c].wait()

        def mix_rows(step, carry, c=c):
            start = pl.multiple_of(c * chunk + step * ROWS, ROWS)
            for i in range(ROWS):
                t = start + i
                first = gates_ref[0, t] * back_ref[where_ref[0, t]].astype(F32)
                sum_ref[i] = first + gates_ref[1, t] * back_ref[where_ref[1, t]].astype(F32)
            update = sum_ref[...].reshape(ROWS, width)
            mixed = near_ref[pl.ds(start, ROWS), :].astype(F32) + update
            out_near[pl.ds(start, ROWS), :] = mixed.astype(BF16)
            return carry

        lax.fori_loop(0, chunk // ROWS, mix_rows, 0)
        sent.append(pltpu.make_async_copy(out_near.at[rows[c]], mixed_ref.at[rows[c]], out_sems.at[c]))
        sent[c].start()
    for copy in sent:
        copy.wait()


def mix(back, tokens, gates, where):
    count, width = tokens.shape
    return pl.pallas_call(
        mix_kernel,
        in_specs=[NEAR, FAR] + [SCALARS] * 2,
        out_specs=FAR,
        out_shape=pltpu.HBM(tokens.shape, BF16),
        scratch_shapes=[
            pltpu.VMEM(tokens.shape, BF16),
            pltpu.VMEM(tokens.shape, BF16),
            pltpu.VMEM((ROWS, width // LANES, LANES), F32),
            pltpu.SemaphoreType.DMA((CHUNKS,)),
            pltpu.SemaphoreType.DMA((CHUNKS,)),
        ],
        compiler_params=params(16),
        name="mix",
    )(kept(back), far(tokens), gates, where)


def everywhere(x):
    for axis in EXPERT[::-1]:
        x = lax.psum(x, axis)
    return x


def exchange(x):
    return lax.all_to_all(x, EXPERT, split_axis=0, concat_axis=0, tiled=True)


def body(
    tokens,
    norm_gain,
    router_weight,
    expert_ids,
    gate_proj,
    up_proj,
    down_proj,
    value_weight,
    value_target,
    recency,
):
    count, width = tokens.shape
    experts = router_weight.shape[1]
    parts = width // LANES
    ids = expert_ids.T
    gain = norm_gain.reshape(1, width)
    weight = value_weight.reshape(1, width).astype(F32)
    received = exchange(route(tokens, gain, ids, experts))
    gates, where, base, scores = gate(tokens, gain, router_weight, ids, weight, down_proj)
    hidden, scored = expert_up(received, gate_proj, up_proj, scores)
    part = exchange(scored.reshape(experts, 1, LANES)).reshape(experts, LANES)
    back = exchange(expert_down(hidden, down_proj))
    values, sums = value(
        part, ids, gates, base, value_target.reshape(1, count), recency.reshape(1, count)
    )
    total = everywhere(sums)
    mixed = mix(back.reshape(experts * SLOTS, parts, LANES), tokens, gates, where)
    return (mixed, values.reshape(count), total[0, 0] / total[0, 1])


def solution(mesh):
    finer = Mesh(mesh.devices.reshape(4, 4, 4, 2), EXPERT)
    in_specs = (
        P(EXPERT, None),
        P(),
        P(),
        P(EXPERT, None),
        P(EXPERT, None, None),
        P(EXPERT, None, None),
        P(EXPERT, None, None),
        P(),
        P(EXPERT),
        P(EXPERT),
    )
    out_specs = (P(EXPERT, None), P(EXPERT), P())
    return jax.shard_map(body, mesh=finer, in_specs=in_specs, out_specs=out_specs, check_vma=False)
```

```python
import jax
import jax.numpy as jnp
from jax import lax
from jax.experimental import pallas as pl
from jax.experimental.pallas import tpu as pltpu
from jax.sharding import Mesh
from jax.sharding import PartitionSpec as P

EXPERT = ("expert_0", "expert_1", "expert_2", "expert_3")
F32 = jnp.float32
BF16 = jnp.bfloat16
I32 = jnp.int32
LANES = 128
SLOTS = 3
ROWS = 16
NORM_ROWS = 32
BLOCK = 128
CHUNKS = 4
MIB = 1024 * 1024
NEAR = pl.BlockSpec(memory_space=pltpu.VMEM)
FAR = pl.BlockSpec(memory_space=pltpu.HBM)


def params(mib):
    return pltpu.CompilerParams(vmem_limit_bytes=mib * MIB)


def cost(flops, moved):
    return pl.CostEstimate(flops=flops, transcendentals=0, bytes_accessed=moved)


def kept(x):
    return pltpu.with_memory_space_constraint(x, pltpu.VMEM)


def far(x):
    return pltpu.with_memory_space_constraint(x, pltpu.HBM)


def start_all(pairs, sems):
    copies = [pltpu.make_async_copy(src, dst, sems.at[i]) for i, (src, dst) in enumerate(pairs)]
    for copy in copies:
        copy.start()
    return copies


def pieces_of(count, pieces):
    size = count // pieces
    return [pl.ds(i * size, size) for i in range(pieces)]


def iota(shape, dim):
    return lax.broadcasted_iota(I32, shape, dim)


def to_row(column):
    count = column.shape[0]
    spread = jnp.where(iota((count, count), 0) == iota((count, count), 1), column, jnp.zeros_like(column))
    return jnp.sum(spread, axis=0, keepdims=True)


def slots_of(ids_ref, experts):
    count = ids_ref.shape[1]
    hits = [iota((experts, count), 0) == ids_ref[k:k + 1, :] for k in range(2)]
    named = jnp.where(hits[0] | hits[1], 1.0, 0.0).astype(BF16)
    before = jnp.where(iota((count, count), 0) < iota((count, count), 1), 1.0, 0.0).astype(BF16)
    rank = jnp.dot(named, before, preferred_element_type=F32)
    return hits, rank


def norm(wide, gain):
    inverse = lax.rsqrt(jnp.mean(wide * wide, axis=1, keepdims=True) + 1e-05)
    return (wide * inverse * gain).astype(BF16)


def route_kernel(
    tok_ref, gain_ref, ids_ref, out_ref,
    near_ref, gain_near, ids_near, tall_ref, piece_ref, index_ref, index_smem, sems, out_sems, index_sem,
):
    count, width = tok_ref.shape
    parts = width // LANES
    experts = out_ref.shape[0]
    copies = start_all(
        [(ids_ref, ids_near), (gain_ref, gain_near)]
        + [(tok_ref.at[rows], near_ref.at[rows]) for rows in pieces_of(count, CHUNKS)],
        sems,
    )
    copies[0].wait()
    hits, rank = slots_of(ids_near, experts)
    named = hits[0] | hits[1]
    token = (iota((8, count), 1) - count).astype(F32).astype(BF16)
    for s in range(SLOTS):
        chosen = jnp.where(named & (rank == s), 1.0, 0.0).astype(BF16)
        source = lax.dot_general(token, chosen, (((1,), (1,)), ((), ())), preferred_element_type=F32)
        index_ref[s:s + 1, :] = source[0:1].astype(I32) + count
    index_ref[SLOTS:, :] = jnp.zeros((8 - SLOTS, experts), I32)
    index_copy = pltpu.make_async_copy(index_ref, index_smem, index_sem)
    index_copy.start()
    tall_ref[count] = jnp.zeros((parts, LANES), BF16)
    copies[1].wait()
    gain = gain_near[...]
    chunk = count // CHUNKS
    for c in range(CHUNKS):
        copies[2 + c].wait()

        def norm_rows(step, carry, c=c):
            start = pl.multiple_of(c * chunk + step * NORM_ROWS, NORM_ROWS)
            normed = norm(near_ref[pl.ds(start, NORM_ROWS), :].astype(F32), gain)
            tall_ref[pl.ds(start, NORM_ROWS)] = normed.astype(F32).reshape(NORM_ROWS, parts, LANES).astype(BF16)
            return carry

        lax.fori_loop(0, chunk // NORM_ROWS, norm_rows, 0)
    index_copy.wait()
    chunk = experts // CHUNKS
    sent = []
    for c, rows in enumerate(pieces_of(experts, CHUNKS)):
        def send(step, carry, c=c):
            for i in range(4):
                e = c * chunk + step * 4 + i
                for s in range(SLOTS):
                    piece_ref[e, s * parts:(s + 1) * parts] = tall_ref[index_smem[s, e]]
            return carry

        lax.fori_loop(0, chunk // 4, send, 0)
        sent.append(pltpu.make_async_copy(piece_ref.at[rows], out_ref.at[rows], out_sems.at[c]))
        sent[c].start()
    for copy in sent:
        copy.wait()


def route(tokens, norm_gain, ids, experts):
    count, width = tokens.shape
    parts = width // LANES
    pieces = (experts, SLOTS * parts, LANES)
    return pl.pallas_call(
        route_kernel,
        in_specs=[FAR] * 3,
        out_specs=FAR,
        out_shape=pltpu.HBM(pieces, BF16),
        scratch_shapes=[
            pltpu.VMEM((count, width), BF16),
            pltpu.VMEM(norm_gain.shape, F32),
            pltpu.VMEM(ids.shape, I32),
            pltpu.VMEM((count + 1, parts, LANES), BF16),
            pltpu.VMEM(pieces, BF16),
            pltpu.VMEM((8, experts), I32),
            pltpu.SMEM((8, experts), I32),
            pltpu.SemaphoreType.DMA((2 + CHUNKS,)),
            pltpu.SemaphoreType.DMA((CHUNKS,)),
            pltpu.SemaphoreType.DMA(()),
        ],
        compiler_params=params(16),
        name="route",
    )(far(tokens), far(norm_gain), far(ids))


def gate_kernel(tok_ref, gain_ref, router_ref, ids_ref, gates_ref, where_ref, tall_ref, normed_ref):
    count, width = tok_ref.shape
    parts = width // LANES
    experts = router_ref.shape[1]
    gain = gain_ref[...]

    def norm_rows(step, carry):
        start = pl.multiple_of(step * ROWS, ROWS)
        wide = tok_ref[pl.ds(start, ROWS), :].astype(F32)
        normed_ref[pl.ds(start, ROWS), :] = norm(wide, gain)
        tall_ref[pl.ds(start, ROWS)] = wide.reshape(ROWS, parts, LANES).astype(BF16)
        return carry

    lax.fori_loop(0, count // ROWS, norm_rows, 0)
    hits, rank = slots_of(ids_ref, experts)
    logits = jnp.transpose(jnp.dot(normed_ref[...], router_ref[...], preferred_element_type=F32))
    scores = []
    where_ref[...] = jnp.zeros(where_ref.shape, I32)
    gates_ref[...] = jnp.zeros(gates_ref.shape, F32)
    for k in range(2):
        slot = jnp.sum(jnp.where(hits[k], rank, 0.0), axis=0, keepdims=True).astype(I32)
        where_ref[k:k + 1, :] = ids_ref[k:k + 1, :] * SLOTS + slot
        scores.append(jnp.sum(jnp.where(hits[k], logits, 0.0), axis=0, keepdims=True))
    gates_ref[0:1, :] = jax.nn.sigmoid(scores[0] - scores[1])
    gates_ref[1:2, :] = jax.nn.sigmoid(scores[1] - scores[0])


def gate(tokens, norm_gain, router_weight, ids):
    count, width = tokens.shape
    parts = width // LANES
    return pl.pallas_call(
        gate_kernel,
        in_specs=[NEAR] * 4,
        out_specs=[NEAR] * 3,
        out_shape=[
            jax.ShapeDtypeStruct((8, count), F32),
            jax.ShapeDtypeStruct((8, count), I32),
            pltpu.HBM((count, parts, LANES), BF16),
        ],
        scratch_shapes=[pltpu.VMEM((count, width), BF16)],
        compiler_params=params(16),
        cost_estimate=cost(10**10, 4 * MIB),
        name="gate",
    )(tokens, norm_gain, router_weight, ids)


def ffn_kernel(
    in_ref, gate_ref, up_ref, down_ref, out_ref,
    gate_near, up_near, down_near, wide_ref, hidden_ref, tall_ref, sems, out_sems,
):
    rows, parts, _ = in_ref.shape
    width, hidden = gate_near.shape
    tiles = [slice(start, start + 256) for start in range(0, hidden, 256)]
    pairs = []
    for tile in tiles:
        pairs.append((gate_ref.at[0, :, tile], gate_near.at[:, tile]))
        pairs.append((up_ref.at[0, :, tile], up_near.at[:, tile]))
    for tile in tiles:
        pairs.append((down_ref.at[0, tile, :], down_near.at[tile, :]))
    copies = start_all(pairs, sems)

    def widen(i, carry):
        start = pl.multiple_of(i * ROWS, ROWS)
        tall = in_ref[pl.ds(start, ROWS)].astype(F32)
        wide_ref[pl.ds(start, ROWS), :] = tall.reshape(ROWS, width).astype(BF16)
        return carry

    lax.fori_loop(0, rows // ROWS, widen, 0)
    for i, tile in enumerate(tiles):
        copies[2 * i].wait()
        copies[2 * i + 1].wait()
        x = wide_ref[...]
        gated = jnp.dot(x, gate_near[:, tile], preferred_element_type=F32)
        upped = jnp.dot(x, up_near[:, tile], preferred_element_type=F32)
        hidden_ref[:, tile] = (jax.nn.silu(gated) * upped).astype(BF16)
    for i in range(len(tiles)):
        copies[2 * len(tiles) + i].wait()
    half = width // 2
    sent = []
    for p, start in enumerate(range(0, rows, BLOCK)):
        piece = slice(start, start + BLOCK)
        for side in range(2):
            wide = jnp.dot(
                hidden_ref[piece, :], down_near[:, side * half:(side + 1) * half], preferred_element_type=F32
            )
            tall = wide.reshape(BLOCK, parts // 2, LANES).astype(BF16)
            tall_ref[piece, side * (parts // 2):(side + 1) * (parts // 2)] = tall
        sent.append(pltpu.make_async_copy(tall_ref.at[piece], out_ref.at[piece], out_sems.at[p]))
        sent[p].start()
    for copy in sent:
        copy.wait()


def expert_ffn(received, gate_proj, up_proj, down_proj):
    rows, parts, _ = received.shape
    _, width, hidden = gate_proj.shape
    return pl.pallas_call(
        ffn_kernel,
        in_specs=[NEAR] + [FAR] * 3,
        out_specs=FAR,
        out_shape=pltpu.HBM(received.shape, BF16),
        scratch_shapes=[
            pltpu.VMEM((width, hidden), BF16),
            pltpu.VMEM((width, hidden), BF16),
            pltpu.VMEM((hidden, width), BF16),
            pltpu.VMEM((rows, width), BF16),
            pltpu.VMEM((rows, hidden), BF16),
            pltpu.VMEM((rows, parts, LANES), BF16),
            pltpu.SemaphoreType.DMA((3 * (hidden // 256),)),
            pltpu.SemaphoreType.DMA((rows // BLOCK,)),
        ],
        compiler_params=params(44),
        cost_estimate=cost(6 * rows * width * hidden, 24 * MIB),
        name="ffn",
    )(kept(received), far(gate_proj), far(up_proj), far(down_proj))


def mix_kernel(
    back_ref, token_ref, gates_ref, where_ref, weight_ref, target_ref, recency_ref,
    mixed_ref, values_ref, sums_ref,
    tall_ref, near_ref, score_ref, gates_smem, where_smem, sems, out_sems,
):
    count, parts, _ = token_ref.shape
    rows = pieces_of(count, CHUNKS)
    copies = start_all(
        [(gates_ref, gates_smem), (where_ref, where_smem)] + [(token_ref.at[r], tall_ref.at[r]) for r in rows], sems
    )
    weight = weight_ref[...]
    chunk = count // CHUNKS
    sent = []
    copies[0].wait()
    copies[1].wait()
    for c in range(CHUNKS):
        copies[2 + c].wait()

        def mix_rows(step, carry, c=c):
            for i in range(16):
                t = c * chunk + step * 16 + i
                total = tall_ref[t].astype(F32)
                for k in range(2):
                    total = total + gates_smem[k, t] * back_ref[where_smem[k, t]].astype(F32)
                mixed = total.astype(BF16)
                near_ref[t] = mixed
                scored = mixed.astype(F32) * weight
                score_ref[t] = jnp.sum(scored.reshape(parts // 8, 8, LANES), axis=0)
            return carry

        lax.fori_loop(0, chunk // 16, mix_rows, 0)
        sent.append(pltpu.make_async_copy(near_ref.at[rows[c]], mixed_ref.at[rows[c]], out_sems.at[c]))
        sent[c].start()
    by_lane = jnp.sum(score_ref[...], axis=1)
    values = jnp.tanh(to_row(jnp.sum(by_lane, axis=1, keepdims=True)))
    values_ref[...] = values
    error = values - target_ref[...].astype(F32)
    recency = recency_ref[...]
    weighted = jnp.sum(recency * error * error, axis=1, keepdims=True)
    total = jnp.sum(recency, axis=1, keepdims=True)
    lane = iota(sums_ref.shape, 1)
    sums_ref[...] = jnp.where(lane == 0, weighted, jnp.where(lane == 1, total, 0.0))
    for copy in sent:
        copy.wait()


def mix(back, tall, gates, where, weight, target, recency, devices):
    count, parts, _ = tall.shape
    return pl.pallas_call(
        mix_kernel,
        in_specs=[NEAR, FAR] + [NEAR] * 5,
        out_specs=[FAR] + [NEAR] * 2,
        out_shape=[
            pltpu.HBM(tall.shape, BF16),
            pltpu.VMEM((1, count), F32),
            pltpu.VMEM((devices, LANES), F32),
        ],
        scratch_shapes=[
            pltpu.VMEM((count, parts, LANES), BF16),
            pltpu.VMEM((count, parts, LANES), BF16),
            pltpu.VMEM((count, 8, LANES), F32),
            pltpu.SMEM(gates.shape, F32),
            pltpu.SMEM(where.shape, I32),
            pltpu.SemaphoreType.DMA((2 + CHUNKS,)),
            pltpu.SemaphoreType.DMA((CHUNKS,)),
        ],
        compiler_params=params(16),
        name="mix",
    )(kept(back), far(tall), *[kept(x) for x in (gates, where, weight, target, recency)])


def widen_kernel(tall_ref, out_ref):
    count, width = out_ref.shape

    def widen(i, carry):
        start = pl.multiple_of(i * ROWS, ROWS)
        tall = tall_ref[pl.ds(start, ROWS)].astype(F32)
        out_ref[pl.ds(start, ROWS), :] = tall.reshape(ROWS, width).astype(BF16)
        return carry

    lax.fori_loop(0, count // ROWS, widen, 0)


def widen_rows(tall):
    count, parts, _ = tall.shape
    return pl.pallas_call(
        widen_kernel,
        in_specs=[NEAR],
        out_specs=NEAR,
        out_shape=jax.ShapeDtypeStruct((count, parts * LANES), BF16),
        compiler_params=params(8),
        cost_estimate=cost(10**10, 2 * MIB),
        name="widen",
    )(far(tall))


def exchange(x):
    return lax.all_to_all(x, EXPERT, split_axis=0, concat_axis=0, tiled=True)


def body(
    tokens,
    norm_gain,
    router_weight,
    expert_ids,
    gate_proj,
    up_proj,
    down_proj,
    value_weight,
    value_target,
    recency,
):
    count, width = tokens.shape
    experts = router_weight.shape[1]
    parts = width // LANES
    pieces = (experts, SLOTS * parts, LANES)
    rows = (experts * SLOTS, parts, LANES)
    ids = expert_ids.T
    gain = norm_gain.reshape(1, width)
    received = exchange(route(tokens, gain, ids, experts))
    gates, where, tall = gate(tokens, gain, router_weight, ids)
    produced = expert_ffn(received.reshape(rows), gate_proj, up_proj, down_proj)
    back = exchange(produced.reshape(pieces))
    mixed, values, sums = mix(
        back.reshape(rows), tall, gates, where, value_weight.reshape(parts, LANES).astype(F32),
        value_target.reshape(1, count), recency.reshape(1, count), experts,
    )
    everyone = exchange(sums.reshape(experts, 1, LANES)).reshape(experts, LANES)
    loss = jnp.sum(everyone[:, 0]) / jnp.sum(everyone[:, 1])
    return (widen_rows(mixed), values.reshape(count), loss)


def solution(mesh):
    finer = Mesh(mesh.devices.reshape(4, 4, 4, 2), EXPERT)
    in_specs = (
        P(EXPERT, None),
        P(),
        P(),
        P(EXPERT, None),
        P(EXPERT, None, None),
        P(EXPERT, None, None),
        P(EXPERT, None, None),
        P(),
        P(EXPERT),
        P(EXPERT),
    )
    out_specs = (P(EXPERT, None), P(EXPERT), P())
    return jax.shard_map(body, mesh=finer, in_specs=in_specs, out_specs=out_specs, check_vma=False)
```

```python
import jax
import jax.numpy as jnp
from jax import lax
from jax.experimental import pallas as pl
from jax.experimental.pallas import tpu as pltpu
from jax.sharding import Mesh
from jax.sharding import PartitionSpec as P

EXPERT = ("expert_0", "expert_1", "expert_2", "expert_3")
F32 = jnp.float32
BF16 = jnp.bfloat16
I32 = jnp.int32
LANES = 128
SLOTS = 3
ROWS = 16
NORM_ROWS = 32
BLOCK = 128
CHUNKS = 4
MIB = 1024 * 1024
NEAR = pl.BlockSpec(memory_space=pltpu.VMEM)
SCALARS = pl.BlockSpec(memory_space=pltpu.SMEM)
FAR = pl.BlockSpec(memory_space=pltpu.HBM)


def params(mib):
    return pltpu.CompilerParams(vmem_limit_bytes=mib * MIB)


def cost(flops, moved):
    return pl.CostEstimate(flops=flops, transcendentals=0, bytes_accessed=moved)


def kept(x):
    return pltpu.with_memory_space_constraint(x, pltpu.VMEM)


def far(x):
    return pltpu.with_memory_space_constraint(x, pltpu.HBM)


def start_all(pairs, sems):
    copies = [pltpu.make_async_copy(src, dst, sems.at[i]) for i, (src, dst) in enumerate(pairs)]
    for copy in copies:
        copy.start()
    return copies


def pieces_of(count, pieces):
    size = count // pieces
    return [pl.ds(i * size, size) for i in range(pieces)]


def iota(shape, dim):
    return lax.broadcasted_iota(I32, shape, dim)


def to_row(column):
    count = column.shape[0]
    spread = jnp.where(iota((count, count), 0) == iota((count, count), 1), column, jnp.zeros_like(column))
    return jnp.sum(spread, axis=0, keepdims=True)


def slots_of(ids_ref, experts):
    count = ids_ref.shape[1]
    hits = [iota((experts, count), 0) == ids_ref[k:k + 1, :] for k in range(2)]
    named = jnp.where(hits[0] | hits[1], 1.0, 0.0).astype(BF16)
    before = jnp.where(iota((count, count), 0) < iota((count, count), 1), 1.0, 0.0).astype(BF16)
    rank = jnp.dot(named, before, preferred_element_type=F32)
    return hits, rank


def norm(wide, gain):
    inverse = lax.rsqrt(jnp.mean(wide * wide, axis=1, keepdims=True) + 1e-05)
    return (wide * inverse * gain).astype(BF16)


def route_kernel(
    tok_ref, gain_ref, ids_ref, out_ref,
    near_ref, gain_near, ids_near, tall_ref, piece_ref, index_ref, index_smem, sems, out_sems, index_sem,
):
    count, width = tok_ref.shape
    parts = width // LANES
    experts = out_ref.shape[0]
    copies = start_all(
        [(ids_ref, ids_near), (gain_ref, gain_near)]
        + [(tok_ref.at[rows], near_ref.at[rows]) for rows in pieces_of(count, CHUNKS)],
        sems,
    )
    copies[0].wait()
    hits, rank = slots_of(ids_near, experts)
    named = hits[0] | hits[1]
    token = (iota((8, count), 1) - count).astype(F32).astype(BF16)
    for s in range(SLOTS):
        chosen = jnp.where(named & (rank == s), 1.0, 0.0).astype(BF16)
        source = lax.dot_general(token, chosen, (((1,), (1,)), ((), ())), preferred_element_type=F32)
        index_ref[s:s + 1, :] = source[0:1].astype(I32) + count
    index_ref[SLOTS:, :] = jnp.zeros((8 - SLOTS, experts), I32)
    index_copy = pltpu.make_async_copy(index_ref, index_smem, index_sem)
    index_copy.start()
    tall_ref[count] = jnp.zeros((parts, LANES), BF16)
    copies[1].wait()
    gain = gain_near[...]
    chunk = count // CHUNKS
    for c in range(CHUNKS):
        copies[2 + c].wait()

        def norm_rows(step, carry, c=c):
            start = pl.multiple_of(c * chunk + step * NORM_ROWS, NORM_ROWS)
            normed = norm(near_ref[pl.ds(start, NORM_ROWS), :].astype(F32), gain)
            tall_ref[pl.ds(start, NORM_ROWS)] = normed.astype(F32).reshape(NORM_ROWS, parts, LANES).astype(BF16)
            return carry

        lax.fori_loop(0, chunk // NORM_ROWS, norm_rows, 0)
    index_copy.wait()
    chunk = experts // CHUNKS
    sent = []
    for c, rows in enumerate(pieces_of(experts, CHUNKS)):
        def send(step, carry, c=c):
            for i in range(4):
                e = c * chunk + step * 4 + i
                for s in range(SLOTS):
                    piece_ref[e, s * parts:(s + 1) * parts] = tall_ref[index_smem[s, e]]
            return carry

        lax.fori_loop(0, chunk // 4, send, 0)
        sent.append(pltpu.make_async_copy(piece_ref.at[rows], out_ref.at[rows], out_sems.at[c]))
        sent[c].start()
    for copy in sent:
        copy.wait()


def route(tokens, norm_gain, ids, experts):
    count, width = tokens.shape
    parts = width // LANES
    pieces = (experts, SLOTS * parts, LANES)
    return pl.pallas_call(
        route_kernel,
        in_specs=[FAR] * 3,
        out_specs=FAR,
        out_shape=pltpu.HBM(pieces, BF16),
        scratch_shapes=[
            pltpu.VMEM((count, width), BF16),
            pltpu.VMEM(norm_gain.shape, F32),
            pltpu.VMEM(ids.shape, I32),
            pltpu.VMEM((count + 1, parts, LANES), BF16),
            pltpu.VMEM(pieces, BF16),
            pltpu.VMEM((8, experts), I32),
            pltpu.SMEM((8, experts), I32),
            pltpu.SemaphoreType.DMA((2 + CHUNKS,)),
            pltpu.SemaphoreType.DMA((CHUNKS,)),
            pltpu.SemaphoreType.DMA(()),
        ],
        compiler_params=params(16),
        name="route",
    )(far(tokens), far(norm_gain), far(ids))


def gate_kernel(
    *refs,
):
    inputs, (gates_ref, where_ref, base_ref), scratch = refs[:5], refs[5:8], refs[8:]
    tok_ref, gain_ref, router_ref, ids_ref, weight_ref, normed_ref, score_ref, sems = scratch
    for copy in start_all(zip(inputs, scratch[:5]), sems):
        copy.wait()
    count, width = tok_ref.shape
    experts = router_ref.shape[1]
    gain = gain_ref[...]
    weight = weight_ref[...]

    def norm_rows(step, carry):
        start = pl.multiple_of(step * ROWS, ROWS)
        wide = tok_ref[pl.ds(start, ROWS), :].astype(F32)
        normed_ref[pl.ds(start, ROWS), :] = norm(wide, gain)
        score_ref[pl.ds(start, ROWS), :] = jnp.sum(wide * weight, axis=1, keepdims=True)
        return carry

    lax.fori_loop(0, count // ROWS, norm_rows, 0)
    base_ref[...] = to_row(score_ref[...])
    hits, rank = slots_of(ids_ref, experts)
    logits = jnp.transpose(jnp.dot(normed_ref[...], router_ref[...], preferred_element_type=F32))
    scores = []
    where_ref[...] = jnp.zeros(where_ref.shape, I32)
    gates_ref[...] = jnp.zeros(gates_ref.shape, F32)
    for k in range(2):
        slot = jnp.sum(jnp.where(hits[k], rank, 0.0), axis=0, keepdims=True).astype(I32)
        where_ref[k:k + 1, :] = ids_ref[k:k + 1, :] * SLOTS + slot
        scores.append(jnp.sum(jnp.where(hits[k], logits, 0.0), axis=0, keepdims=True))
    gates_ref[0:1, :] = jax.nn.sigmoid(scores[0] - scores[1])
    gates_ref[1:2, :] = jax.nn.sigmoid(scores[1] - scores[0])


def gate(tokens, norm_gain, router_weight, ids, weight):
    count, width = tokens.shape
    inputs = (tokens, norm_gain, router_weight, ids, weight)
    return pl.pallas_call(
        gate_kernel,
        in_specs=[FAR] * 5,
        out_specs=[NEAR] * 3,
        out_shape=[
            jax.ShapeDtypeStruct((8, count), F32),
            jax.ShapeDtypeStruct((8, count), I32),
            jax.ShapeDtypeStruct((1, count), F32),
        ],
        scratch_shapes=[pltpu.VMEM(x.shape, x.dtype) for x in inputs]
        + [pltpu.VMEM((count, width), BF16), pltpu.VMEM((count, 1), F32), pltpu.SemaphoreType.DMA((5,))],
        compiler_params=params(16),
        cost_estimate=cost(10**10, 4 * MIB),
        name="gate",
    )(*[far(x) for x in inputs])


def ffn_kernel(
    in_ref, gate_ref, up_ref, down_ref, out_ref,
    both_near, down_near, wide_ref, hidden_ref, tall_ref, part_ref, sems, out_sems,
):
    rows, parts, _ = in_ref.shape
    hidden, width = down_near.shape
    half = width // 2
    tile = both_near.shape[2] // 2
    blocks = [(0, slice(0, half)), (0, slice(half, width))]
    blocks += [(i, slice(0, width)) for i in range(1, hidden // tile)]
    pairs = []
    for i, deep in blocks:
        columns = slice(i * tile, (i + 1) * tile)
        pairs.append((gate_ref.at[0, deep, columns], both_near.at[i, deep, 0:tile]))
        pairs.append((up_ref.at[0, deep, columns], both_near.at[i, deep, tile:2 * tile]))
    copies = start_all(pairs + [(down_ref.at[0], down_near)], sems)

    def widen(i, carry):
        start = pl.multiple_of(i * ROWS, ROWS)
        tall = in_ref[pl.ds(start, ROWS)].astype(F32)
        wide_ref[pl.ds(start, ROWS), :] = tall.reshape(ROWS, width).astype(BF16)
        return carry

    lax.fori_loop(0, rows // ROWS, widen, 0)
    for n, (i, deep) in enumerate(blocks):
        copies[2 * n].wait()
        copies[2 * n + 1].wait()
        both = jnp.dot(wide_ref[:, deep], both_near[i, deep, :], preferred_element_type=F32)
        if n == 0:
            part_ref[...] = both
            continue
        if n == 1:
            both = both + part_ref[...]
        hidden_ref[:, i * tile:(i + 1) * tile] = (jax.nn.silu(both[:, :tile]) * both[:, tile:]).astype(BF16)
    copies[-1].wait()
    sent = []
    for p, start in enumerate(range(0, rows, BLOCK)):
        piece = slice(start, start + BLOCK)
        for side in range(2):
            wide = jnp.dot(
                hidden_ref[piece, :], down_near[:, side * half:(side + 1) * half], preferred_element_type=F32
            )
            tall = wide.reshape(BLOCK, parts // 2, LANES).astype(BF16)
            tall_ref[piece, side * (parts // 2):(side + 1) * (parts // 2)] = tall
        sent.append(pltpu.make_async_copy(tall_ref.at[piece], out_ref.at[piece], out_sems.at[p]))
        sent[p].start()
    for copy in sent:
        copy.wait()


def expert_ffn(received, gate_proj, up_proj, down_proj):
    rows, parts, _ = received.shape
    _, width, hidden = gate_proj.shape
    tile = 256
    return pl.pallas_call(
        ffn_kernel,
        in_specs=[NEAR] + [FAR] * 3,
        out_specs=FAR,
        out_shape=pltpu.HBM(received.shape, BF16),
        scratch_shapes=[
            pltpu.VMEM((hidden // tile, width, 2 * tile), BF16),
            pltpu.VMEM((hidden, width), BF16),
            pltpu.VMEM((rows, width), BF16),
            pltpu.VMEM((rows, hidden), BF16),
            pltpu.VMEM((rows, parts, LANES), BF16),
            pltpu.VMEM((rows, 2 * tile), F32),
            pltpu.SemaphoreType.DMA((2 * (hidden // tile) + 3,)),
            pltpu.SemaphoreType.DMA((rows // BLOCK,)),
        ],
        compiler_params=params(48),
        cost_estimate=cost(6 * rows * width * hidden, 24 * MIB),
        name="ffn",
    )(kept(received), far(gate_proj), far(up_proj), far(down_proj))


def value_kernel(
    back_ref, gates_ref, where_ref, base_ref, weight_ref, target_ref, recency_ref,
    values_ref, sums_ref, score_ref, gates_smem, where_smem, sems,
):
    count = base_ref.shape[1]
    parts = weight_ref.shape[0]
    for copy in start_all([(gates_ref, gates_smem), (where_ref, where_smem)], sems):
        copy.wait()
    weight = weight_ref[...]

    def score_rows(step, carry):
        for i in range(16):
            t = step * 16 + i
            first = gates_smem[0, t] * back_ref[where_smem[0, t]].astype(F32)
            mixed = first + gates_smem[1, t] * back_ref[where_smem[1, t]].astype(F32)
            score_ref[t] = jnp.sum((mixed * weight).reshape(parts // 8, 8, LANES), axis=0)
        return carry

    lax.fori_loop(0, count // 16, score_rows, 0)
    by_lane = jnp.sum(score_ref[...], axis=1)
    values = jnp.tanh(base_ref[...] + to_row(jnp.sum(by_lane, axis=1, keepdims=True)))
    values_ref[...] = values
    error = values - target_ref[...].astype(F32)
    recency = recency_ref[...]
    weighted = jnp.sum(recency * error * error, axis=1, keepdims=True)
    total = jnp.sum(recency, axis=1, keepdims=True)
    lane = iota(sums_ref.shape, 1)
    sums_ref[...] = jnp.where(lane == 0, weighted, jnp.where(lane == 1, total, 0.0))


def value(back, gates, where, base, weight, target, recency, devices):
    count = base.shape[1]
    return pl.pallas_call(
        value_kernel,
        in_specs=[NEAR] * 7,
        out_specs=[NEAR] * 2,
        out_shape=[pltpu.VMEM(base.shape, F32), pltpu.VMEM((devices, LANES), F32)],
        scratch_shapes=[
            pltpu.VMEM((count, 8, LANES), F32),
            pltpu.SMEM(gates.shape, F32),
            pltpu.SMEM(where.shape, I32),
            pltpu.SemaphoreType.DMA((2,)),
        ],
        compiler_params=params(8),
        name="value",
    )(*[kept(x) for x in (back, gates, where, base, weight, target, recency)])


def mix_kernel(
    back_ref, token_ref, gates_ref, where_ref, mixed_ref, near_ref, out_near, sum_ref, sems, out_sems
):
    count, width = token_ref.shape
    parts = width // LANES
    rows = pieces_of(count, CHUNKS)
    copies = start_all([(token_ref.at[r], near_ref.at[r]) for r in rows], sems)
    chunk = count // CHUNKS
    sent = []
    for c in range(CHUNKS):
        copies[c].wait()

        def mix_rows(step, carry, c=c):
            start = pl.multiple_of(c * chunk + step * ROWS, ROWS)
            for i in range(ROWS):
                t = start + i
                first = gates_ref[0, t] * back_ref[where_ref[0, t]].astype(F32)
                sum_ref[i] = first + gates_ref[1, t] * back_ref[where_ref[1, t]].astype(F32)
            update = sum_ref[...].reshape(ROWS, width)
            mixed = near_ref[pl.ds(start, ROWS), :].astype(F32) + update
            out_near[pl.ds(start, ROWS), :] = mixed.astype(BF16)
            return carry

        lax.fori_loop(0, chunk // ROWS, mix_rows, 0)
        sent.append(pltpu.make_async_copy(out_near.at[rows[c]], mixed_ref.at[rows[c]], out_sems.at[c]))
        sent[c].start()
    for copy in sent:
        copy.wait()


def mix(back, tokens, gates, where):
    count, width = tokens.shape
    return pl.pallas_call(
        mix_kernel,
        in_specs=[NEAR, FAR] + [SCALARS] * 2,
        out_specs=FAR,
        out_shape=pltpu.HBM(tokens.shape, BF16),
        scratch_shapes=[
            pltpu.VMEM(tokens.shape, BF16),
            pltpu.VMEM(tokens.shape, BF16),
            pltpu.VMEM((ROWS, width // LANES, LANES), F32),
            pltpu.SemaphoreType.DMA((CHUNKS,)),
            pltpu.SemaphoreType.DMA((CHUNKS,)),
        ],
        compiler_params=params(16),
        cost_estimate=cost(10**10, 6 * MIB),
        name="mix",
    )(kept(back), far(tokens), gates, where)


def exchange(x):
    return lax.all_to_all(x, EXPERT, split_axis=0, concat_axis=0, tiled=True)


def body(
    tokens,
    norm_gain,
    router_weight,
    expert_ids,
    gate_proj,
    up_proj,
    down_proj,
    value_weight,
    value_target,
    recency,
):
    count, width = tokens.shape
    experts = router_weight.shape[1]
    parts = width // LANES
    pieces = (experts, SLOTS * parts, LANES)
    rows = (experts * SLOTS, parts, LANES)
    ids = expert_ids.T
    gain = norm_gain.reshape(1, width)
    received = exchange(route(tokens, gain, ids, experts))
    weight = value_weight.astype(F32)
    gates, where, base = gate(tokens, gain, router_weight, ids, weight.reshape(1, width))
    produced = expert_ffn(received.reshape(rows), gate_proj, up_proj, down_proj)
    back = exchange(produced.reshape(pieces)).reshape(rows)
    values, sums = value(
        back, gates, where, base, weight.reshape(parts, LANES),
        value_target.reshape(1, count), recency.reshape(1, count), experts,
    )
    everyone = exchange(sums.reshape(experts, 1, LANES)).reshape(experts, LANES)
    mixed = mix(back, tokens, gates, where)
    return (mixed, values.reshape(count), jnp.sum(everyone[:, 0]) / jnp.sum(everyone[:, 1]))


def solution(mesh):
    finer = Mesh(mesh.devices.reshape(4, 4, 4, 2), EXPERT)
    in_specs = (
        P(EXPERT, None),
        P(),
        P(),
        P(EXPERT, None),
        P(EXPERT, None, None),
        P(EXPERT, None, None),
        P(EXPERT, None, None),
        P(),
        P(EXPERT),
        P(EXPERT),
    )
    out_specs = (P(EXPERT, None), P(EXPERT), P())
    return jax.shard_map(body, mesh=finer, in_specs=in_specs, out_specs=out_specs, check_vma=False)
```

```python
import jax
import jax.numpy as jnp
from jax import lax
from jax.experimental import pallas as pl
from jax.experimental.pallas import tpu as pltpu
from jax.sharding import Mesh
from jax.sharding import PartitionSpec as P

EXPERT = ("expert_0", "expert_1", "expert_2", "expert_3")
F32 = jnp.float32
BF16 = jnp.bfloat16
I32 = jnp.int32
LANES = 128
SLOTS = 3
ROWS = 16
NORM_ROWS = 32
BLOCK = 128
CHUNKS = 4
MIB = 1024 * 1024
NEAR = pl.BlockSpec(memory_space=pltpu.VMEM)
SCALARS = pl.BlockSpec(memory_space=pltpu.SMEM)
FAR = pl.BlockSpec(memory_space=pltpu.HBM)


def params(mib):
    return pltpu.CompilerParams(vmem_limit_bytes=mib * MIB)


def cost(flops, moved):
    return pl.CostEstimate(flops=flops, transcendentals=0, bytes_accessed=moved)


def kept(x):
    return pltpu.with_memory_space_constraint(x, pltpu.VMEM)


def far(x):
    return pltpu.with_memory_space_constraint(x, pltpu.HBM)


def start_all(pairs, sems):
    copies = [pltpu.make_async_copy(src, dst, sems.at[i]) for i, (src, dst) in enumerate(pairs)]
    for copy in copies:
        copy.start()
    return copies


def pieces_of(count, pieces):
    size = count // pieces
    return [pl.ds(i * size, size) for i in range(pieces)]


def iota(shape, dim):
    return lax.broadcasted_iota(I32, shape, dim)


def to_row(column):
    count = column.shape[0]
    spread = jnp.where(iota((count, count), 0) == iota((count, count), 1), column, jnp.zeros_like(column))
    return jnp.sum(spread, axis=0, keepdims=True)


def slots_of(ids_ref, experts):
    count = ids_ref.shape[1]
    hits = [iota((experts, count), 0) == ids_ref[k:k + 1, :] for k in range(2)]
    named = jnp.where(hits[0] | hits[1], 1.0, 0.0).astype(BF16)
    before = jnp.where(iota((count, count), 0) < iota((count, count), 1), 1.0, 0.0).astype(BF16)
    rank = jnp.dot(named, before, preferred_element_type=F32)
    return hits, rank


def norm(wide, gain):
    inverse = lax.rsqrt(jnp.mean(wide * wide, axis=1, keepdims=True) + 1e-05)
    return (wide * inverse * gain).astype(BF16)


def route_kernel(
    tok_ref, gain_ref, ids_ref, out_ref,
    near_ref, gain_near, ids_near, tall_ref, piece_ref, index_ref, index_smem, sems, out_sems, index_sem,
):
    count, width = tok_ref.shape
    parts = width // LANES
    experts = out_ref.shape[0]
    copies = start_all(
        [(ids_ref, ids_near), (gain_ref, gain_near)]
        + [(tok_ref.at[rows], near_ref.at[rows]) for rows in pieces_of(count, CHUNKS)],
        sems,
    )
    copies[0].wait()
    hits, rank = slots_of(ids_near, experts)
    named = hits[0] | hits[1]
    token = (iota((8, count), 1) - count).astype(F32).astype(BF16)
    for s in range(SLOTS):
        chosen = jnp.where(named & (rank == s), 1.0, 0.0).astype(BF16)
        source = lax.dot_general(token, chosen, (((1,), (1,)), ((), ())), preferred_element_type=F32)
        index_ref[s:s + 1, :] = source[0:1].astype(I32) + count
    index_ref[SLOTS:, :] = jnp.zeros((8 - SLOTS, experts), I32)
    index_copy = pltpu.make_async_copy(index_ref, index_smem, index_sem)
    index_copy.start()
    tall_ref[count] = jnp.zeros((parts, LANES), BF16)
    copies[1].wait()
    gain = gain_near[...]
    chunk = count // CHUNKS
    for c in range(CHUNKS):
        copies[2 + c].wait()

        def norm_rows(step, carry, c=c):
            start = pl.multiple_of(c * chunk + step * NORM_ROWS, NORM_ROWS)
            normed = norm(near_ref[pl.ds(start, NORM_ROWS), :].astype(F32), gain)
            tall_ref[pl.ds(start, NORM_ROWS)] = normed.astype(F32).reshape(NORM_ROWS, parts, LANES).astype(BF16)
            return carry

        lax.fori_loop(0, chunk // NORM_ROWS, norm_rows, 0)
    index_copy.wait()
    chunk = experts // CHUNKS
    sent = []
    for c, rows in enumerate(pieces_of(experts, CHUNKS)):
        def send(step, carry, c=c):
            for i in range(4):
                e = c * chunk + step * 4 + i
                for s in range(SLOTS):
                    piece_ref[e, s * parts:(s + 1) * parts] = tall_ref[index_smem[s, e]]
            return carry

        lax.fori_loop(0, chunk // 4, send, 0)
        sent.append(pltpu.make_async_copy(piece_ref.at[rows], out_ref.at[rows], out_sems.at[c]))
        sent[c].start()
    for copy in sent:
        copy.wait()


def route(tokens, norm_gain, ids, experts):
    count, width = tokens.shape
    parts = width // LANES
    pieces = (experts, SLOTS * parts, LANES)
    return pl.pallas_call(
        route_kernel,
        in_specs=[FAR] * 3,
        out_specs=FAR,
        out_shape=pltpu.HBM(pieces, BF16),
        scratch_shapes=[
            pltpu.VMEM((count, width), BF16),
            pltpu.VMEM(norm_gain.shape, F32),
            pltpu.VMEM(ids.shape, I32),
            pltpu.VMEM((count + 1, parts, LANES), BF16),
            pltpu.VMEM(pieces, BF16),
            pltpu.VMEM((8, experts), I32),
            pltpu.SMEM((8, experts), I32),
            pltpu.SemaphoreType.DMA((2 + CHUNKS,)),
            pltpu.SemaphoreType.DMA((CHUNKS,)),
            pltpu.SemaphoreType.DMA(()),
        ],
        compiler_params=params(16),
        name="route",
    )(far(tokens), far(norm_gain), far(ids))


def gate_kernel(
    *refs,
):
    inputs, (gates_out, where_out, base_ref), scratch = refs[:5], refs[5:8], refs[8:]
    tok_ref, gain_ref, router_ref, ids_ref, weight_ref, normed_ref, score_ref, gates_ref, where_ref, sems = scratch
    for copy in start_all(zip(inputs, scratch[:5]), sems):
        copy.wait()
    count, width = tok_ref.shape
    experts = router_ref.shape[1]
    gain = gain_ref[...]
    weight = weight_ref[...]

    def norm_rows(step, carry):
        start = pl.multiple_of(step * ROWS, ROWS)
        wide = tok_ref[pl.ds(start, ROWS), :].astype(F32)
        normed_ref[pl.ds(start, ROWS), :] = norm(wide, gain)
        score_ref[pl.ds(start, ROWS), :] = jnp.sum(wide * weight, axis=1, keepdims=True)
        return carry

    lax.fori_loop(0, count // ROWS, norm_rows, 0)
    base_ref[...] = to_row(score_ref[...])
    hits, rank = slots_of(ids_ref, experts)
    logits = jnp.transpose(jnp.dot(normed_ref[...], router_ref[...], preferred_element_type=F32))
    scores = []
    where_ref[...] = jnp.zeros(where_ref.shape, I32)
    gates_ref[...] = jnp.zeros(gates_ref.shape, F32)
    for k in range(2):
        slot = jnp.sum(jnp.where(hits[k], rank, 0.0), axis=0, keepdims=True).astype(I32)
        where_ref[k:k + 1, :] = ids_ref[k:k + 1, :] * SLOTS + slot
        scores.append(jnp.sum(jnp.where(hits[k], logits, 0.0), axis=0, keepdims=True))
    gates_ref[0:1, :] = jax.nn.sigmoid(scores[0] - scores[1])
    gates_ref[1:2, :] = jax.nn.sigmoid(scores[1] - scores[0])
    for copy in start_all([(gates_ref, gates_out), (where_ref, where_out)], sems):
        copy.wait()


def gate(tokens, norm_gain, router_weight, ids, weight):
    count, width = tokens.shape
    inputs = (tokens, norm_gain, router_weight, ids, weight)
    return pl.pallas_call(
        gate_kernel,
        in_specs=[FAR] * 5,
        out_specs=[SCALARS, SCALARS, NEAR],
        out_shape=[
            pltpu.SMEM((8, count), F32),
            pltpu.SMEM((8, count), I32),
            jax.ShapeDtypeStruct((1, count), F32),
        ],
        scratch_shapes=[pltpu.VMEM(x.shape, x.dtype) for x in inputs]
        + [pltpu.VMEM((count, width), BF16), pltpu.VMEM((count, 1), F32)]
        + [pltpu.VMEM((8, count), F32), pltpu.VMEM((8, count), I32), pltpu.SemaphoreType.DMA((5,))],
        compiler_params=params(16),
        cost_estimate=cost(10**10, 4 * MIB),
        name="gate",
    )(*[far(x) for x in inputs])


def ffn_kernel(
    in_ref, gate_ref, up_ref, down_ref, out_ref,
    both_near, down_near, wide_ref, hidden_ref, tall_ref, part_ref, sems, out_sems,
):
    rows, parts, _ = in_ref.shape
    hidden, width = down_near.shape
    half = width // 2
    tile = both_near.shape[2] // 2
    blocks = [(0, slice(0, half)), (0, slice(half, width))]
    blocks += [(i, slice(0, width)) for i in range(1, hidden // tile)]
    pairs = []
    for i, deep in blocks:
        columns = slice(i * tile, (i + 1) * tile)
        pairs.append((gate_ref.at[0, deep, columns], both_near.at[i, deep, 0:tile]))
        pairs.append((up_ref.at[0, deep, columns], both_near.at[i, deep, tile:2 * tile]))
    copies = start_all(pairs + [(down_ref.at[0], down_near)], sems)

    def widen(i, carry):
        start = pl.multiple_of(i * ROWS, ROWS)
        tall = in_ref[pl.ds(start, ROWS)].astype(F32)
        wide_ref[pl.ds(start, ROWS), :] = tall.reshape(ROWS, width).astype(BF16)
        return carry

    lax.fori_loop(0, rows // ROWS, widen, 0)

    def join(i):
        both = part_ref.at[i % 2]
        hidden_ref[:, i * tile:(i + 1) * tile] = (jax.nn.silu(both[:, :tile]) * both[:, tile:]).astype(BF16)

    for n, (i, deep) in enumerate(blocks):
        copies[2 * n].wait()
        copies[2 * n + 1].wait()
        both = jnp.dot(wide_ref[:, deep], both_near[i, deep, :], preferred_element_type=F32)
        if n == 1:
            part_ref[0] += both
            continue
        part_ref[i % 2] = both
        if i > 0:
            join(i - 1)
    join(hidden // tile - 1)
    copies[-1].wait()
    sent = []
    for p, start in enumerate(range(0, rows, BLOCK)):
        piece = slice(start, start + BLOCK)
        for side in range(2):
            wide = jnp.dot(
                hidden_ref[piece, :], down_near[:, side * half:(side + 1) * half], preferred_element_type=F32
            )
            tall = wide.reshape(BLOCK, parts // 2, LANES).astype(BF16)
            at = (piece, slice(side * (parts // 2), (side + 1) * (parts // 2)))
            tall_ref[at] = tall
            sent.append(pltpu.make_async_copy(tall_ref.at[at], out_ref.at[at], out_sems.at[2 * p + side]))
            sent[-1].start()
    for copy in sent:
        copy.wait()


def expert_ffn(received, gate_proj, up_proj, down_proj):
    rows, parts, _ = received.shape
    _, width, hidden = gate_proj.shape
    tile = 256
    return pl.pallas_call(
        ffn_kernel,
        in_specs=[NEAR] + [FAR] * 3,
        out_specs=FAR,
        out_shape=pltpu.HBM(received.shape, BF16),
        scratch_shapes=[
            pltpu.VMEM((hidden // tile, width, 2 * tile), BF16),
            pltpu.VMEM((hidden, width), BF16),
            pltpu.VMEM((rows, width), BF16),
            pltpu.VMEM((rows, hidden), BF16),
            pltpu.VMEM((rows, parts, LANES), BF16),
            pltpu.VMEM((2, rows, 2 * tile), F32),
            pltpu.SemaphoreType.DMA((2 * (hidden // tile) + 3,)),
            pltpu.SemaphoreType.DMA((2 * (rows // BLOCK),)),
        ],
        compiler_params=params(48),
        cost_estimate=cost(6 * rows * width * hidden, 24 * MIB),
        name="ffn",
    )(kept(received), far(gate_proj), far(up_proj), far(down_proj))


def value_kernel(
    back_ref, gates_smem, where_smem, base_ref, weight_ref, target_ref, recency_ref,
    values_ref, sums_ref, score_ref,
):
    count = base_ref.shape[1]
    parts = weight_ref.shape[0]
    weight = weight_ref[...]

    def score_rows(step, carry):
        for i in range(16):
            t = step * 16 + i
            first = gates_smem[0, t] * back_ref[where_smem[0, t]].astype(F32)
            mixed = first + gates_smem[1, t] * back_ref[where_smem[1, t]].astype(F32)
            score_ref[t] = jnp.sum((mixed * weight).reshape(parts // 8, 8, LANES), axis=0)
        return carry

    lax.fori_loop(0, count // 16, score_rows, 0)
    by_lane = jnp.sum(score_ref[...], axis=1)
    values = jnp.tanh(base_ref[...] + to_row(jnp.sum(by_lane, axis=1, keepdims=True)))
    values_ref[...] = values
    error = values - target_ref[...].astype(F32)
    recency = recency_ref[...]
    weighted = jnp.sum(recency * error * error, axis=1, keepdims=True)
    total = jnp.sum(recency, axis=1, keepdims=True)
    lane = iota(sums_ref.shape, 1)
    sums_ref[...] = jnp.where(lane == 0, weighted, jnp.where(lane == 1, total, 0.0))


def value(back, gates, where, base, weight, target, recency, devices):
    count = base.shape[1]
    return pl.pallas_call(
        value_kernel,
        in_specs=[NEAR, SCALARS, SCALARS] + [NEAR] * 4,
        out_specs=[NEAR] * 2,
        out_shape=[pltpu.VMEM(base.shape, F32), pltpu.VMEM((devices, LANES), F32)],
        scratch_shapes=[pltpu.VMEM((count, 8, LANES), F32)],
        compiler_params=params(8),
        name="value",
    )(kept(back), gates, where, *[kept(x) for x in (base, weight, target, recency)])


def mix_kernel(
    back_ref, token_ref, gates_ref, where_ref, mixed_ref, near_ref, out_near, sum_ref, sems, out_sems
):
    count, width = token_ref.shape
    parts = width // LANES
    rows = pieces_of(count, CHUNKS)
    copies = start_all([(token_ref.at[r], near_ref.at[r]) for r in rows], sems)
    chunk = count // CHUNKS
    sent = []
    for c in range(CHUNKS):
        copies[c].wait()

        def mix_rows(step, carry, c=c):
            start = pl.multiple_of(c * chunk + step * ROWS, ROWS)
            for i in range(ROWS):
                t = start + i
                first = gates_ref[0, t] * back_ref[where_ref[0, t]].astype(F32)
                sum_ref[i] = first + gates_ref[1, t] * back_ref[where_ref[1, t]].astype(F32)
            update = sum_ref[...].reshape(ROWS, width)
            mixed = near_ref[pl.ds(start, ROWS), :].astype(F32) + update
            out_near[pl.ds(start, ROWS), :] = mixed.astype(BF16)
            return carry

        lax.fori_loop(0, chunk // ROWS, mix_rows, 0)
        sent.append(pltpu.make_async_copy(out_near.at[rows[c]], mixed_ref.at[rows[c]], out_sems.at[c]))
        sent[c].start()
    for copy in sent:
        copy.wait()


def mix(back, tokens, gates, where):
    count, width = tokens.shape
    return pl.pallas_call(
        mix_kernel,
        in_specs=[NEAR, FAR] + [SCALARS] * 2,
        out_specs=FAR,
        out_shape=pltpu.HBM(tokens.shape, BF16),
        scratch_shapes=[
            pltpu.VMEM(tokens.shape, BF16),
            pltpu.VMEM(tokens.shape, BF16),
            pltpu.VMEM((ROWS, width // LANES, LANES), F32),
            pltpu.SemaphoreType.DMA((CHUNKS,)),
            pltpu.SemaphoreType.DMA((CHUNKS,)),
        ],
        compiler_params=params(16),
        cost_estimate=cost(10**10, 6 * MIB),
        name="mix",
    )(kept(back), far(tokens), gates, where)


def exchange(x):
    return lax.all_to_all(x, EXPERT, split_axis=0, concat_axis=0, tiled=True)


def body(
    tokens,
    norm_gain,
    router_weight,
    expert_ids,
    gate_proj,
    up_proj,
    down_proj,
    value_weight,
    value_target,
    recency,
):
    count, width = tokens.shape
    experts = router_weight.shape[1]
    parts = width // LANES
    pieces = (experts, SLOTS * parts, LANES)
    rows = (experts * SLOTS, parts, LANES)
    ids = expert_ids.T
    gain = norm_gain.reshape(1, width)
    received = exchange(route(tokens, gain, ids, experts))
    weight = value_weight.astype(F32)
    gates, where, base = gate(tokens, gain, router_weight, ids, weight.reshape(1, width))
    produced = expert_ffn(received.reshape(rows), gate_proj, up_proj, down_proj)
    back = exchange(produced.reshape(pieces)).reshape(rows)
    values, sums = value(
        back, gates, where, base, weight.reshape(parts, LANES),
        value_target.reshape(1, count), recency.reshape(1, count), experts,
    )
    everyone = exchange(sums.reshape(experts, 1, LANES)).reshape(experts, LANES)
    mixed = mix(back, tokens, gates, where)
    return (mixed, values.reshape(count), jnp.sum(everyone[:, 0]) / jnp.sum(everyone[:, 1]))


def solution(mesh):
    finer = Mesh(mesh.devices.reshape(4, 4, 4, 2), EXPERT)
    in_specs = (
        P(EXPERT, None),
        P(),
        P(),
        P(EXPERT, None),
        P(EXPERT, None, None),
        P(EXPERT, None, None),
        P(EXPERT, None, None),
        P(),
        P(EXPERT),
        P(EXPERT),
    )
    out_specs = (P(EXPERT, None), P(EXPERT), P())
    return jax.shard_map(body, mesh=finer, in_specs=in_specs, out_specs=out_specs, check_vma=False)
```

```python
import jax
import jax.numpy as jnp
from jax import lax
from jax.experimental import pallas as pl
from jax.experimental.pallas import tpu as pltpu
from jax.sharding import Mesh
from jax.sharding import PartitionSpec as P

EXPERT = ("expert_0", "expert_1", "expert_2", "expert_3")
F32 = jnp.float32
BF16 = jnp.bfloat16
I32 = jnp.int32
LANES = 128
SLOTS = 3
ROWS = 16
NORM_ROWS = 32
BLOCK = 128
CHUNKS = 4
MIB = 1024 * 1024
NEAR = pl.BlockSpec(memory_space=pltpu.VMEM)
SCALARS = pl.BlockSpec(memory_space=pltpu.SMEM)
FAR = pl.BlockSpec(memory_space=pltpu.HBM)


def params(mib):
    return pltpu.CompilerParams(vmem_limit_bytes=mib * MIB)


def cost(flops, moved):
    return pl.CostEstimate(flops=flops, transcendentals=0, bytes_accessed=moved)


def kept(x):
    return pltpu.with_memory_space_constraint(x, pltpu.VMEM)


def far(x):
    return pltpu.with_memory_space_constraint(x, pltpu.HBM)


def start_all(pairs, sems):
    copies = [pltpu.make_async_copy(src, dst, sems.at[i]) for i, (src, dst) in enumerate(pairs)]
    for copy in copies:
        copy.start()
    return copies


def pieces_of(count, pieces):
    size = count // pieces
    return [pl.ds(i * size, size) for i in range(pieces)]


def iota(shape, dim):
    return lax.broadcasted_iota(I32, shape, dim)


def to_row(column):
    count = column.shape[0]
    spread = jnp.where(iota((count, count), 0) == iota((count, count), 1), column, jnp.zeros_like(column))
    return jnp.sum(spread, axis=0, keepdims=True)


def slots_of(ids_ref, experts):
    count = ids_ref.shape[1]
    hits = [iota((experts, count), 0) == ids_ref[k:k + 1, :] for k in range(2)]
    named = jnp.where(hits[0] | hits[1], 1.0, 0.0).astype(BF16)
    before = jnp.where(iota((count, count), 0) < iota((count, count), 1), 1.0, 0.0).astype(BF16)
    rank = jnp.dot(named, before, preferred_element_type=F32)
    return hits, rank


def norm(wide, gain):
    inverse = lax.rsqrt(jnp.mean(wide * wide, axis=1, keepdims=True) + 1e-05)
    return (wide * inverse * gain).astype(BF16)


def route_kernel(
    tok_ref, gain_ref, ids_ref, out_ref,
    near_ref, gain_near, ids_near, tall_ref, piece_ref, index_ref, index_smem, sems, out_sems, index_sem,
):
    count, width = tok_ref.shape
    parts = width // LANES
    experts = out_ref.shape[0]
    copies = start_all(
        [(ids_ref, ids_near), (gain_ref, gain_near)]
        + [(tok_ref.at[rows], near_ref.at[rows]) for rows in pieces_of(count, CHUNKS)],
        sems,
    )
    copies[0].wait()
    hits, rank = slots_of(ids_near, experts)
    named = hits[0] | hits[1]
    token = (iota((8, count), 1) - count).astype(F32).astype(BF16)
    for s in range(SLOTS):
        chosen = jnp.where(named & (rank == s), 1.0, 0.0).astype(BF16)
        source = lax.dot_general(token, chosen, (((1,), (1,)), ((), ())), preferred_element_type=F32)
        index_ref[s:s + 1, :] = source[0:1].astype(I32) + count
    index_ref[SLOTS:, :] = jnp.zeros((8 - SLOTS, experts), I32)
    index_copy = pltpu.make_async_copy(index_ref, index_smem, index_sem)
    index_copy.start()
    tall_ref[count] = jnp.zeros((parts, LANES), BF16)
    copies[1].wait()
    gain = gain_near[...]
    chunk = count // CHUNKS
    for c in range(CHUNKS):
        copies[2 + c].wait()

        def norm_rows(step, carry, c=c):
            start = pl.multiple_of(c * chunk + step * NORM_ROWS, NORM_ROWS)
            normed = norm(near_ref[pl.ds(start, NORM_ROWS), :].astype(F32), gain)
            tall_ref[pl.ds(start, NORM_ROWS)] = normed.astype(F32).reshape(NORM_ROWS, parts, LANES).astype(BF16)
            return carry

        lax.fori_loop(0, chunk // NORM_ROWS, norm_rows, 0)
    index_copy.wait()
    chunk = experts // CHUNKS
    sent = []
    for c, rows in enumerate(pieces_of(experts, CHUNKS)):
        def send(step, carry, c=c):
            for i in range(4):
                e = c * chunk + step * 4 + i
                for s in range(SLOTS):
                    piece_ref[e, s * parts:(s + 1) * parts] = tall_ref[index_smem[s, e]]
            return carry

        lax.fori_loop(0, chunk // 4, send, 0)
        sent.append(pltpu.make_async_copy(piece_ref.at[rows], out_ref.at[rows], out_sems.at[c]))
        sent[c].start()
    for copy in sent:
        copy.wait()


def route(tokens, norm_gain, ids, experts):
    count, width = tokens.shape
    parts = width // LANES
    pieces = (experts, SLOTS * parts, LANES)
    return pl.pallas_call(
        route_kernel,
        in_specs=[FAR] * 3,
        out_specs=FAR,
        out_shape=pltpu.HBM(pieces, BF16),
        scratch_shapes=[
            pltpu.VMEM((count, width), BF16),
            pltpu.VMEM(norm_gain.shape, F32),
            pltpu.VMEM(ids.shape, I32),
            pltpu.VMEM((count + 1, parts, LANES), BF16),
            pltpu.VMEM(pieces, BF16),
            pltpu.VMEM((8, experts), I32),
            pltpu.SMEM((8, experts), I32),
            pltpu.SemaphoreType.DMA((2 + CHUNKS,)),
            pltpu.SemaphoreType.DMA((CHUNKS,)),
            pltpu.SemaphoreType.DMA(()),
        ],
        compiler_params=params(16),
        name="route",
    )(far(tokens), far(norm_gain), far(ids))


def gate_kernel(
    *refs,
):
    inputs, (gates_out, where_out, base_ref), scratch = refs[:5], refs[5:8], refs[8:]
    tok_ref, gain_ref, router_ref, ids_ref, weight_ref, normed_ref, score_ref, gates_ref, where_ref, sems = scratch
    for copy in start_all(zip(inputs, scratch[:5]), sems):
        copy.wait()
    count, width = tok_ref.shape
    experts = router_ref.shape[1]
    gain = gain_ref[...]
    weight = weight_ref[...]

    def norm_rows(step, carry):
        start = pl.multiple_of(step * ROWS, ROWS)
        wide = tok_ref[pl.ds(start, ROWS), :].astype(F32)
        normed_ref[pl.ds(start, ROWS), :] = norm(wide, gain)
        score_ref[pl.ds(start, ROWS), :] = jnp.sum(wide * weight, axis=1, keepdims=True)
        return carry

    lax.fori_loop(0, count // ROWS, norm_rows, 0)
    base_ref[...] = to_row(score_ref[...])
    hits, rank = slots_of(ids_ref, experts)
    logits = jnp.transpose(jnp.dot(normed_ref[...], router_ref[...], preferred_element_type=F32))
    scores = []
    where_ref[...] = jnp.zeros(where_ref.shape, I32)
    gates_ref[...] = jnp.zeros(gates_ref.shape, F32)
    for k in range(2):
        slot = jnp.sum(jnp.where(hits[k], rank, 0.0), axis=0, keepdims=True).astype(I32)
        where_ref[k:k + 1, :] = ids_ref[k:k + 1, :] * SLOTS + slot
        scores.append(jnp.sum(jnp.where(hits[k], logits, 0.0), axis=0, keepdims=True))
    gates_ref[0:1, :] = jax.nn.sigmoid(scores[0] - scores[1])
    gates_ref[1:2, :] = jax.nn.sigmoid(scores[1] - scores[0])
    for copy in start_all([(gates_ref, gates_out), (where_ref, where_out)], sems):
        copy.wait()


def gate(tokens, norm_gain, router_weight, ids, weight):
    count, width = tokens.shape
    inputs = (tokens, norm_gain, router_weight, ids, weight)
    return pl.pallas_call(
        gate_kernel,
        in_specs=[FAR] * 5,
        out_specs=[SCALARS, SCALARS, NEAR],
        out_shape=[
            pltpu.SMEM((8, count), F32),
            pltpu.SMEM((8, count), I32),
            jax.ShapeDtypeStruct((1, count), F32),
        ],
        scratch_shapes=[pltpu.VMEM(x.shape, x.dtype) for x in inputs]
        + [pltpu.VMEM((count, width), BF16), pltpu.VMEM((count, 1), F32)]
        + [pltpu.VMEM((8, count), F32), pltpu.VMEM((8, count), I32), pltpu.SemaphoreType.DMA((5,))],
        compiler_params=params(16),
        cost_estimate=cost(10**10, 4 * MIB),
        name="gate",
    )(*[far(x) for x in inputs])


def ffn_kernel(
    in_ref, gate_ref, up_ref, down_ref, out_ref,
    both_near, down_near, wide_ref, hidden_ref, tall_ref, part_ref, sems, out_sems,
):
    rows, parts, _ = in_ref.shape
    hidden, width = down_near.shape
    half = width // 2
    tile = both_near.shape[2] // 2
    blocks = [(0, slice(0, half)), (0, slice(half, width))]
    blocks += [(i, slice(0, width)) for i in range(1, hidden // tile)]
    pairs = []
    for i, deep in blocks:
        columns = slice(i * tile, (i + 1) * tile)
        pairs.append((gate_ref.at[0, deep, columns], both_near.at[i, deep, 0:tile]))
        pairs.append((up_ref.at[0, deep, columns], both_near.at[i, deep, tile:2 * tile]))
    copies = start_all(pairs + [(down_ref.at[0], down_near)], sems)

    def widen(i, carry):
        start = pl.multiple_of(i * ROWS, ROWS)
        tall = in_ref[pl.ds(start, ROWS)].astype(F32)
        wide_ref[pl.ds(start, ROWS), :] = tall.reshape(ROWS, width).astype(BF16)
        return carry

    lax.fori_loop(0, rows // ROWS, widen, 0)

    def join(i):
        both = part_ref.at[i % 2]
        hidden_ref[:, i * tile:(i + 1) * tile] = (jax.nn.silu(both[:, :tile]) * both[:, tile:]).astype(BF16)

    for n, (i, deep) in enumerate(blocks):
        copies[2 * n].wait()
        copies[2 * n + 1].wait()
        both = jnp.dot(wide_ref[:, deep], both_near[i, deep, :], preferred_element_type=F32)
        if n == 1:
            part_ref[0] += both
            continue
        part_ref[i % 2] = both
        if i > 0:
            join(i - 1)
    join(hidden // tile - 1)
    copies[-1].wait()
    sent = []
    for p, start in enumerate(range(0, rows, BLOCK)):
        piece = slice(start, start + BLOCK)
        for side in range(2):
            wide = jnp.dot(
                hidden_ref[piece, :], down_near[:, side * half:(side + 1) * half], preferred_element_type=F32
            )
            tall = wide.reshape(BLOCK, parts // 2, LANES).astype(BF16)
            at = (piece, slice(side * (parts // 2), (side + 1) * (parts // 2)))
            tall_ref[at] = tall
            sent.append(pltpu.make_async_copy(tall_ref.at[at], out_ref.at[at], out_sems.at[2 * p + side]))
            sent[-1].start()
    for copy in sent:
        copy.wait()


def expert_ffn(received, gate_proj, up_proj, down_proj):
    rows, parts, _ = received.shape
    _, width, hidden = gate_proj.shape
    tile = 256
    return pl.pallas_call(
        ffn_kernel,
        in_specs=[NEAR] + [FAR] * 3,
        out_specs=FAR,
        out_shape=pltpu.HBM(received.shape, BF16),
        scratch_shapes=[
            pltpu.VMEM((hidden // tile, width, 2 * tile), BF16),
            pltpu.VMEM((hidden, width), BF16),
            pltpu.VMEM((rows, width), BF16),
            pltpu.VMEM((rows, hidden), BF16),
            pltpu.VMEM((rows, parts, LANES), BF16),
            pltpu.VMEM((2, rows, 2 * tile), F32),
            pltpu.SemaphoreType.DMA((2 * (hidden // tile) + 3,)),
            pltpu.SemaphoreType.DMA((2 * (rows // BLOCK),)),
        ],
        compiler_params=params(48),
        cost_estimate=cost(6 * rows * width * hidden, 24 * MIB),
        name="ffn",
    )(kept(received), far(gate_proj), far(up_proj), far(down_proj))


def value_kernel(
    back_ref, gates_smem, where_smem, base_ref, weight_ref, target_ref, recency_ref,
    values_ref, sums_ref, score_ref,
):
    count = base_ref.shape[1]
    parts = weight_ref.shape[0]
    weight = weight_ref[...]

    def score_rows(step, carry):
        for i in range(16):
            t = step * 16 + i
            first = gates_smem[0, t] * back_ref[where_smem[0, t]].astype(F32)
            mixed = first + gates_smem[1, t] * back_ref[where_smem[1, t]].astype(F32)
            score_ref[t] = jnp.sum((mixed * weight).reshape(parts // 8, 8, LANES), axis=0)
        return carry

    lax.fori_loop(0, count // 16, score_rows, 0)
    by_lane = jnp.sum(score_ref[...], axis=1)
    values = jnp.tanh(base_ref[...] + to_row(jnp.sum(by_lane, axis=1, keepdims=True)))
    values_ref[...] = values
    error = values - target_ref[...].astype(F32)
    recency = recency_ref[...]
    weighted = jnp.sum(recency * error * error, axis=1, keepdims=True)
    total = jnp.sum(recency, axis=1, keepdims=True)
    lane = iota(sums_ref.shape, 1)
    sums_ref[...] = jnp.where(lane == 0, weighted, jnp.where(lane == 1, total, 0.0))


def value(back, gates, where, base, weight, target, recency, devices):
    count = base.shape[1]
    return pl.pallas_call(
        value_kernel,
        in_specs=[NEAR, SCALARS, SCALARS] + [NEAR] * 4,
        out_specs=[NEAR] * 2,
        out_shape=[pltpu.VMEM(base.shape, F32), pltpu.VMEM((devices, LANES), F32)],
        scratch_shapes=[pltpu.VMEM((count, 8, LANES), F32)],
        compiler_params=params(8),
        name="value",
    )(kept(back), gates, where, *[kept(x) for x in (base, weight, target, recency)])


def mix_kernel(
    back_ref, token_ref, gates_ref, where_ref, mixed_ref, near_ref, out_near, sum_ref, sems, out_sems
):
    count, width = token_ref.shape
    parts = width // LANES
    rows = pieces_of(count, CHUNKS)
    copies = start_all([(token_ref.at[r], near_ref.at[r]) for r in rows], sems)
    chunk = count // CHUNKS
    sent = []
    for c in range(CHUNKS):
        copies[c].wait()

        def mix_rows(step, carry, c=c):
            start = pl.multiple_of(c * chunk + step * ROWS, ROWS)
            for i in range(ROWS):
                t = start + i
                first = gates_ref[0, t] * back_ref[where_ref[0, t]].astype(F32)
                sum_ref[i] = first + gates_ref[1, t] * back_ref[where_ref[1, t]].astype(F32)
            update = sum_ref[...].reshape(ROWS, width)
            mixed = near_ref[pl.ds(start, ROWS), :].astype(F32) + update
            out_near[pl.ds(start, ROWS), :] = mixed.astype(BF16)
            return carry

        lax.fori_loop(0, chunk // ROWS, mix_rows, 0)
        sent.append(pltpu.make_async_copy(out_near.at[rows[c]], mixed_ref.at[rows[c]], out_sems.at[c]))
        sent[c].start()
    for copy in sent:
        copy.wait()


def mix(back, tokens, gates, where):
    count, width = tokens.shape
    return pl.pallas_call(
        mix_kernel,
        in_specs=[NEAR, FAR] + [SCALARS] * 2,
        out_specs=FAR,
        out_shape=pltpu.HBM(tokens.shape, BF16),
        scratch_shapes=[
            pltpu.VMEM(tokens.shape, BF16),
            pltpu.VMEM(tokens.shape, BF16),
            pltpu.VMEM((ROWS, width // LANES, LANES), F32),
            pltpu.SemaphoreType.DMA((CHUNKS,)),
            pltpu.SemaphoreType.DMA((CHUNKS,)),
        ],
        compiler_params=params(16),
        cost_estimate=cost(10**10, 6 * MIB),
        name="mix",
    )(kept(back), far(tokens), gates, where)


def loss_kernel(sums_ref, loss_ref):
    total = jnp.sum(sums_ref[...], axis=0, keepdims=True)
    loss_ref[...] = total[:, 0:1] / total[:, 1:2]


def loss_of(sums):
    return pl.pallas_call(
        loss_kernel,
        in_specs=[NEAR],
        out_specs=NEAR,
        out_shape=jax.ShapeDtypeStruct((1, 1), F32),
        compiler_params=params(4),
        name="loss",
    )(kept(sums))


def exchange(x):
    return lax.all_to_all(x, EXPERT, split_axis=0, concat_axis=0, tiled=True)


def body(
    tokens,
    norm_gain,
    router_weight,
    expert_ids,
    gate_proj,
    up_proj,
    down_proj,
    value_weight,
    value_target,
    recency,
):
    count, width = tokens.shape
    experts = router_weight.shape[1]
    parts = width // LANES
    pieces = (experts, SLOTS * parts, LANES)
    rows = (experts * SLOTS, parts, LANES)
    ids = expert_ids.T
    gain = norm_gain.reshape(1, width)
    received = exchange(route(tokens, gain, ids, experts))
    weight = value_weight.astype(F32)
    gates, where, base = gate(tokens, gain, router_weight, ids, weight.reshape(1, width))
    produced = expert_ffn(received.reshape(rows), gate_proj, up_proj, down_proj)
    back = exchange(produced.reshape(pieces)).reshape(rows)
    values, sums = value(
        back, gates, where, base, weight.reshape(parts, LANES),
        value_target.reshape(1, count), recency.reshape(1, count), experts,
    )
    everyone = exchange(sums.reshape(experts, 1, LANES)).reshape(experts, LANES)
    mixed = mix(back, tokens, gates, where)
    return (mixed, values.reshape(count), loss_of(everyone).reshape(()))


def solution(mesh):
    finer = Mesh(mesh.devices.reshape(4, 4, 4, 2), EXPERT)
    in_specs = (
        P(EXPERT, None),
        P(),
        P(),
        P(EXPERT, None),
        P(EXPERT, None, None),
        P(EXPERT, None, None),
        P(EXPERT, None, None),
        P(),
        P(EXPERT),
        P(EXPERT),
    )
    out_specs = (P(EXPERT, None), P(EXPERT), P())
    return jax.shard_map(body, mesh=finer, in_specs=in_specs, out_specs=out_specs, check_vma=False)
```

```python
import jax
import jax.numpy as jnp
from jax import lax
from jax.experimental import pallas as pl
from jax.experimental.pallas import tpu as pltpu
from jax.sharding import Mesh
from jax.sharding import PartitionSpec as P

EXPERT = ("expert_0", "expert_1", "expert_2", "expert_3")
F32 = jnp.float32
BF16 = jnp.bfloat16
I32 = jnp.int32
LANES = 128
SLOTS = 3
ROWS = 16
NORM_ROWS = 32
BLOCK = 128
CHUNKS = 4
MIB = 1024 * 1024
NEAR = pl.BlockSpec(memory_space=pltpu.VMEM)
SCALARS = pl.BlockSpec(memory_space=pltpu.SMEM)
FAR = pl.BlockSpec(memory_space=pltpu.HBM)


def params(mib):
    return pltpu.CompilerParams(vmem_limit_bytes=mib * MIB)


def cost(flops, moved):
    return pl.CostEstimate(flops=flops, transcendentals=0, bytes_accessed=moved)


def kept(x):
    return pltpu.with_memory_space_constraint(x, pltpu.VMEM)


def far(x):
    return pltpu.with_memory_space_constraint(x, pltpu.HBM)


def start_all(pairs, sems):
    copies = [pltpu.make_async_copy(src, dst, sems.at[i]) for i, (src, dst) in enumerate(pairs)]
    for copy in copies:
        copy.start()
    return copies


def pieces_of(count, pieces):
    size = count // pieces
    return [pl.ds(i * size, size) for i in range(pieces)]


def iota(shape, dim):
    return lax.broadcasted_iota(I32, shape, dim)


def to_row(column):
    count = column.shape[0]
    spread = jnp.where(iota((count, count), 0) == iota((count, count), 1), column, jnp.zeros_like(column))
    return jnp.sum(spread, axis=0, keepdims=True)


def slots_of(ids_ref, experts):
    count = ids_ref.shape[1]
    hits = [iota((experts, count), 0) == ids_ref[k:k + 1, :] for k in range(2)]
    named = jnp.where(hits[0] | hits[1], 1.0, 0.0).astype(BF16)
    before = jnp.where(iota((count, count), 0) < iota((count, count), 1), 1.0, 0.0).astype(BF16)
    rank = jnp.dot(named, before, preferred_element_type=F32)
    return hits, rank


def place_of(expert):
    return (expert & 1) * 64 + ((expert >> 1) & 3) * 16 + ((expert >> 3) & 3) * 4 + (expert >> 5)


def expert_at(place):
    return (place & 3) * 32 + ((place >> 2) & 3) * 8 + ((place >> 4) & 3) * 2 + (place >> 6)


def norm(wide, gain):
    inverse = lax.rsqrt(jnp.mean(wide * wide, axis=1, keepdims=True) + 1e-05)
    return (wide * inverse * gain).astype(BF16)


def route_kernel(
    tok_ref, gain_ref, ids_ref, out_ref,
    near_ref, gain_near, ids_near, tall_ref, piece_ref, index_ref, index_smem, sems, out_sems, index_sem,
):
    count, width = tok_ref.shape
    parts = width // LANES
    experts = out_ref.shape[0]
    copies = start_all(
        [(ids_ref, ids_near), (gain_ref, gain_near)]
        + [(tok_ref.at[rows], near_ref.at[rows]) for rows in pieces_of(count, CHUNKS)],
        sems,
    )
    copies[0].wait()
    hits, rank = slots_of(ids_near, experts)
    named = hits[0] | hits[1]
    token = (iota((8, count), 1) - count).astype(F32).astype(BF16)
    for s in range(SLOTS):
        chosen = jnp.where(named & (rank == s), 1.0, 0.0).astype(BF16)
        source = lax.dot_general(token, chosen, (((1,), (1,)), ((), ())), preferred_element_type=F32)
        index_ref[s:s + 1, :] = source[0:1].astype(I32) + count
    index_ref[SLOTS:, :] = jnp.zeros((8 - SLOTS, experts), I32)
    index_copy = pltpu.make_async_copy(index_ref, index_smem, index_sem)
    index_copy.start()
    tall_ref[count] = jnp.zeros((parts, LANES), BF16)
    copies[1].wait()
    gain = gain_near[...]
    chunk = count // CHUNKS
    for c in range(CHUNKS):
        copies[2 + c].wait()

        def norm_rows(step, carry, c=c):
            start = pl.multiple_of(c * chunk + step * NORM_ROWS, NORM_ROWS)
            normed = norm(near_ref[pl.ds(start, NORM_ROWS), :].astype(F32), gain)
            tall_ref[pl.ds(start, NORM_ROWS)] = normed.astype(F32).reshape(NORM_ROWS, parts, LANES).astype(BF16)
            return carry

        lax.fori_loop(0, chunk // NORM_ROWS, norm_rows, 0)
    index_copy.wait()
    chunk = experts // CHUNKS
    sent = []
    for c, rows in enumerate(pieces_of(experts, CHUNKS)):
        def send(step, carry, c=c):
            for i in range(4):
                e = c * chunk + step * 4 + i
                for s in range(SLOTS):
                    piece_ref[e, s * parts:(s + 1) * parts] = tall_ref[index_smem[s, expert_at(e)]]
            return carry

        lax.fori_loop(0, chunk // 4, send, 0)
        sent.append(pltpu.make_async_copy(piece_ref.at[rows], out_ref.at[rows], out_sems.at[c]))
        sent[c].start()
    for copy in sent:
        copy.wait()


def route(tokens, norm_gain, ids, experts):
    count, width = tokens.shape
    parts = width // LANES
    pieces = (experts, SLOTS * parts, LANES)
    return pl.pallas_call(
        route_kernel,
        in_specs=[FAR] * 3,
        out_specs=FAR,
        out_shape=pltpu.HBM(pieces, BF16),
        scratch_shapes=[
            pltpu.VMEM((count, width), BF16),
            pltpu.VMEM(norm_gain.shape, F32),
            pltpu.VMEM(ids.shape, I32),
            pltpu.VMEM((count + 1, parts, LANES), BF16),
            pltpu.VMEM(pieces, BF16),
            pltpu.VMEM((8, experts), I32),
            pltpu.SMEM((8, experts), I32),
            pltpu.SemaphoreType.DMA((2 + CHUNKS,)),
            pltpu.SemaphoreType.DMA((CHUNKS,)),
            pltpu.SemaphoreType.DMA(()),
        ],
        compiler_params=params(16),
        name="route",
    )(far(tokens), far(norm_gain), far(ids))


def gate_kernel(
    *refs,
):
    inputs, (gates_out, where_out, base_ref), scratch = refs[:5], refs[5:8], refs[8:]
    tok_ref, gain_ref, router_ref, ids_ref, weight_ref, normed_ref, score_ref, gates_ref, where_ref, sems = scratch
    for copy in start_all(zip(inputs, scratch[:5]), sems):
        copy.wait()
    count, width = tok_ref.shape
    experts = router_ref.shape[1]
    gain = gain_ref[...]
    weight = weight_ref[...]

    def norm_rows(step, carry):
        start = pl.multiple_of(step * ROWS, ROWS)
        wide = tok_ref[pl.ds(start, ROWS), :].astype(F32)
        normed_ref[pl.ds(start, ROWS), :] = norm(wide, gain)
        score_ref[pl.ds(start, ROWS), :] = jnp.sum(wide * weight, axis=1, keepdims=True)
        return carry

    lax.fori_loop(0, count // ROWS, norm_rows, 0)
    base_ref[...] = to_row(score_ref[...])
    hits, rank = slots_of(ids_ref, experts)
    logits = jnp.transpose(jnp.dot(normed_ref[...], router_ref[...], preferred_element_type=F32))
    scores = []
    where_ref[...] = jnp.zeros(where_ref.shape, I32)
    gates_ref[...] = jnp.zeros(gates_ref.shape, F32)
    for k in range(2):
        slot = jnp.sum(jnp.where(hits[k], rank, 0.0), axis=0, keepdims=True).astype(I32)
        where_ref[k:k + 1, :] = place_of(ids_ref[k:k + 1, :]) * SLOTS + slot
        scores.append(jnp.sum(jnp.where(hits[k], logits, 0.0), axis=0, keepdims=True))
    gates_ref[0:1, :] = jax.nn.sigmoid(scores[0] - scores[1])
    gates_ref[1:2, :] = jax.nn.sigmoid(scores[1] - scores[0])
    for copy in start_all([(gates_ref, gates_out), (where_ref, where_out)], sems):
        copy.wait()


def gate(tokens, norm_gain, router_weight, ids, weight):
    count, width = tokens.shape
    inputs = (tokens, norm_gain, router_weight, ids, weight)
    return pl.pallas_call(
        gate_kernel,
        in_specs=[FAR] * 5,
        out_specs=[SCALARS, SCALARS, NEAR],
        out_shape=[
            pltpu.SMEM((8, count), F32),
            pltpu.SMEM((8, count), I32),
            jax.ShapeDtypeStruct((1, count), F32),
        ],
        scratch_shapes=[pltpu.VMEM(x.shape, x.dtype) for x in inputs]
        + [pltpu.VMEM((count, width), BF16), pltpu.VMEM((count, 1), F32)]
        + [pltpu.VMEM((8, count), F32), pltpu.VMEM((8, count), I32), pltpu.SemaphoreType.DMA((5,))],
        compiler_params=params(16),
        cost_estimate=cost(10**10, 4 * MIB),
        name="gate",
    )(*[far(x) for x in inputs])


def ffn_kernel(
    in_ref, gate_ref, up_ref, down_ref, out_ref,
    both_near, down_near, wide_ref, hidden_ref, tall_ref, part_ref, sems, out_sems,
):
    rows, parts, _ = in_ref.shape
    hidden, width = down_near.shape
    half = width // 2
    tile = both_near.shape[2] // 2
    blocks = [(0, slice(0, half)), (0, slice(half, width))]
    blocks += [(i, slice(0, width)) for i in range(1, hidden // tile)]
    pairs = []
    for i, deep in blocks:
        columns = slice(i * tile, (i + 1) * tile)
        pairs.append((gate_ref.at[0, deep, columns], both_near.at[i, deep, 0:tile]))
        pairs.append((up_ref.at[0, deep, columns], both_near.at[i, deep, tile:2 * tile]))
    copies = start_all(pairs + [(down_ref.at[0], down_near)], sems)

    def widen(i, carry):
        start = pl.multiple_of(i * ROWS, ROWS)
        tall = in_ref[pl.ds(start, ROWS)].astype(F32)
        wide_ref[pl.ds(start, ROWS), :] = tall.reshape(ROWS, width).astype(BF16)
        return carry

    lax.fori_loop(0, rows // ROWS, widen, 0)

    def join(i):
        both = part_ref.at[i % 2]
        hidden_ref[:, i * tile:(i + 1) * tile] = (jax.nn.silu(both[:, :tile]) * both[:, tile:]).astype(BF16)

    for n, (i, deep) in enumerate(blocks):
        copies[2 * n].wait()
        copies[2 * n + 1].wait()
        both = jnp.dot(wide_ref[:, deep], both_near[i, deep, :], preferred_element_type=F32)
        if n == 1:
            part_ref[0] += both
            continue
        part_ref[i % 2] = both
        if i > 0:
            join(i - 1)
    join(hidden // tile - 1)
    copies[-1].wait()
    sent = []
    for p, start in enumerate(range(0, rows, BLOCK)):
        piece = slice(start, start + BLOCK)
        for side in range(2):
            wide = jnp.dot(
                hidden_ref[piece, :], down_near[:, side * half:(side + 1) * half], preferred_element_type=F32
            )
            tall = wide.reshape(BLOCK, parts // 2, LANES).astype(BF16)
            at = (piece, slice(side * (parts // 2), (side + 1) * (parts // 2)))
            tall_ref[at] = tall
            sent.append(pltpu.make_async_copy(tall_ref.at[at], out_ref.at[at], out_sems.at[2 * p + side]))
            sent[-1].start()
    for copy in sent:
        copy.wait()


def expert_ffn(received, gate_proj, up_proj, down_proj):
    rows, parts, _ = received.shape
    _, width, hidden = gate_proj.shape
    tile = 256
    return pl.pallas_call(
        ffn_kernel,
        in_specs=[NEAR] + [FAR] * 3,
        out_specs=FAR,
        out_shape=pltpu.HBM(received.shape, BF16),
        scratch_shapes=[
            pltpu.VMEM((hidden // tile, width, 2 * tile), BF16),
            pltpu.VMEM((hidden, width), BF16),
            pltpu.VMEM((rows, width), BF16),
            pltpu.VMEM((rows, hidden), BF16),
            pltpu.VMEM((rows, parts, LANES), BF16),
            pltpu.VMEM((2, rows, 2 * tile), F32),
            pltpu.SemaphoreType.DMA((2 * (hidden // tile) + 3,)),
            pltpu.SemaphoreType.DMA((2 * (rows // BLOCK),)),
        ],
        compiler_params=params(48),
        cost_estimate=cost(6 * rows * width * hidden, 24 * MIB),
        name="ffn",
    )(kept(received), far(gate_proj), far(up_proj), far(down_proj))


def value_kernel(
    back_ref, gates_smem, where_smem, base_ref, weight_ref, target_ref, recency_ref,
    values_ref, sums_ref, score_ref,
):
    count = base_ref.shape[1]
    parts = weight_ref.shape[0]
    weight = weight_ref[...]

    def score_rows(step, carry):
        for i in range(16):
            t = step * 16 + i
            first = gates_smem[0, t] * back_ref[where_smem[0, t]].astype(F32)
            mixed = first + gates_smem[1, t] * back_ref[where_smem[1, t]].astype(F32)
            score_ref[t] = jnp.sum((mixed * weight).reshape(parts // 8, 8, LANES), axis=0)
        return carry

    lax.fori_loop(0, count // 16, score_rows, 0)
    by_lane = jnp.sum(score_ref[...], axis=1)
    values = jnp.tanh(base_ref[...] + to_row(jnp.sum(by_lane, axis=1, keepdims=True)))
    values_ref[...] = values
    error = values - target_ref[...].astype(F32)
    recency = recency_ref[...]
    weighted = jnp.sum(recency * error * error, axis=1, keepdims=True)
    total = jnp.sum(recency, axis=1, keepdims=True)
    lane = iota(sums_ref.shape, 1)
    sums_ref[...] = jnp.where(lane == 0, weighted, jnp.where(lane == 1, total, 0.0))


def value(back, gates, where, base, weight, target, recency, devices):
    count = base.shape[1]
    return pl.pallas_call(
        value_kernel,
        in_specs=[NEAR, SCALARS, SCALARS] + [NEAR] * 4,
        out_specs=[NEAR] * 2,
        out_shape=[pltpu.VMEM(base.shape, F32), pltpu.VMEM((devices, LANES), F32)],
        scratch_shapes=[pltpu.VMEM((count, 8, LANES), F32)],
        compiler_params=params(8),
        name="value",
    )(kept(back), gates, where, *[kept(x) for x in (base, weight, target, recency)])


def mix_kernel(
    back_ref, token_ref, gates_ref, where_ref, mixed_ref, near_ref, out_near, sum_ref, sems, out_sems
):
    count, width = token_ref.shape
    parts = width // LANES
    rows = pieces_of(count, CHUNKS)
    copies = start_all([(token_ref.at[r], near_ref.at[r]) for r in rows], sems)
    chunk = count // CHUNKS
    sent = []
    for c in range(CHUNKS):
        copies[c].wait()

        def mix_rows(step, carry, c=c):
            start = pl.multiple_of(c * chunk + step * ROWS, ROWS)
            for i in range(ROWS):
                t = start + i
                first = gates_ref[0, t] * back_ref[where_ref[0, t]].astype(F32)
                sum_ref[i] = first + gates_ref[1, t] * back_ref[where_ref[1, t]].astype(F32)
            update = sum_ref[...].reshape(ROWS, width)
            mixed = near_ref[pl.ds(start, ROWS), :].astype(F32) + update
            out_near[pl.ds(start, ROWS), :] = mixed.astype(BF16)
            return carry

        lax.fori_loop(0, chunk // ROWS, mix_rows, 0)
        sent.append(pltpu.make_async_copy(out_near.at[rows[c]], mixed_ref.at[rows[c]], out_sems.at[c]))
        sent[c].start()
    for copy in sent:
        copy.wait()


def mix(back, tokens, gates, where):
    count, width = tokens.shape
    return pl.pallas_call(
        mix_kernel,
        in_specs=[NEAR, FAR] + [SCALARS] * 2,
        out_specs=FAR,
        out_shape=pltpu.HBM(tokens.shape, BF16),
        scratch_shapes=[
            pltpu.VMEM(tokens.shape, BF16),
            pltpu.VMEM(tokens.shape, BF16),
            pltpu.VMEM((ROWS, width // LANES, LANES), F32),
            pltpu.SemaphoreType.DMA((CHUNKS,)),
            pltpu.SemaphoreType.DMA((CHUNKS,)),
        ],
        compiler_params=params(16),
        cost_estimate=cost(10**10, 6 * MIB),
        name="mix",
    )(kept(back), far(tokens), gates, where)


def loss_kernel(sums_ref, loss_ref):
    total = jnp.sum(sums_ref[...], axis=0, keepdims=True)
    loss_ref[...] = total[:, 0:1] / total[:, 1:2]


def loss_of(sums):
    return pl.pallas_call(
        loss_kernel,
        in_specs=[NEAR],
        out_specs=NEAR,
        out_shape=jax.ShapeDtypeStruct((1, 1), F32),
        compiler_params=params(4),
        name="loss",
    )(kept(sums))


def exchange(x):
    return lax.all_to_all(x, EXPERT[::-1], split_axis=0, concat_axis=0, tiled=True)


def body(
    tokens,
    norm_gain,
    router_weight,
    expert_ids,
    gate_proj,
    up_proj,
    down_proj,
    value_weight,
    value_target,
    recency,
):
    count, width = tokens.shape
    experts = router_weight.shape[1]
    parts = width // LANES
    pieces = (experts, SLOTS * parts, LANES)
    rows = (experts * SLOTS, parts, LANES)
    ids = expert_ids.T
    gain = norm_gain.reshape(1, width)
    received = exchange(route(tokens, gain, ids, experts))
    weight = value_weight.astype(F32)
    gates, where, base = gate(tokens, gain, router_weight, ids, weight.reshape(1, width))
    produced = expert_ffn(received.reshape(rows), gate_proj, up_proj, down_proj)
    back = exchange(produced.reshape(pieces)).reshape(rows)
    values, sums = value(
        back, gates, where, base, weight.reshape(parts, LANES),
        value_target.reshape(1, count), recency.reshape(1, count), experts,
    )
    everyone = exchange(sums.reshape(experts, 1, LANES)).reshape(experts, LANES)
    mixed = mix(back, tokens, gates, where)
    return (mixed, values.reshape(count), loss_of(everyone).reshape(()))


def solution(mesh):
    finer = Mesh(mesh.devices.reshape(4, 4, 4, 2), EXPERT)
    in_specs = (
        P(EXPERT, None),
        P(),
        P(),
        P(EXPERT, None),
        P(EXPERT, None, None),
        P(EXPERT, None, None),
        P(EXPERT, None, None),
        P(),
        P(EXPERT),
        P(EXPERT),
    )
    out_specs = (P(EXPERT, None), P(EXPERT), P())
    return jax.shard_map(body, mesh=finer, in_specs=in_specs, out_specs=out_specs, check_vma=False)
```
